8 devices in a mesh: depth: 2 (over z, y), col: 2 (over x), row: 2 (over core).
Axes of the slice: x: 2, y: 2, z: 1, core: 2. Of those that a mesh axis runs over, the one named last changes fastest.
Arguments:
- x: bfloat16 [96, 256, 4096], P(('depth', 'row'), None, 'col')
- ln_g: float32 [4096], P('col')
- ln_b: float32 [4096], P('col')
- w_qkv: bfloat16 [4096, 12288], P('row', 'col')
- b_qkv: float32 [96, 128], P('col')
- w_o: bfloat16 [4096, 4096], P('row', 'col')
- b_o: float32 [4096], P('col')
- d_y: bfloat16 [96, 256, 4096], P(('depth', 'row'), None, 'col')
Outputs:
- output 1: bfloat16 [96, 256, 4096], P(('depth', 'row'), None, 'col')
- output 2: bfloat16 [96, 256, 4096], P(('depth', 'row'), None, 'col')
- output 3: bfloat16 [4096, 12288], P('row', 'col')
- output 4: float32 [96, 128], P('col')
- output 5: bfloat16 [4096, 4096], P('row', 'col')
- output 6: float32 [4096], P('col')
- output 7: float32 [4096], P('col')
- output 8: float32 [4096], P('col')
All inputs are finite; a program needn't handle non-finite values.
Results may differ from the reference program's by a relative error of at most 0.0135278.
Values are sent between devices in bfloat16 or wider.
A program may use at most 1 GiB of HBM per device.

```python
import jax
import jax.numpy as jnp
from jax import lax

HIDDEN = 4096
NUM_HEADS = 32
SEQ_LEN = 256
NUM_SEQS = 96
COL_BLOCKS = 2
HEAD_DIM = HIDDEN // NUM_HEADS
HEADS_PER_COL = NUM_HEADS // COL_BLOCKS
LN_EPS = 1e-5


def setup_inputs(seed: int = 0) -> dict:
    rng_keys = jax.random.split(jax.random.key(seed), 10)
    act_shape = (NUM_SEQS, SEQ_LEN, HIDDEN)
    feat_ramp = jnp.linspace(-1.5, 1.5, HIDDEN, dtype=jnp.float32)
    base_noise = jax.random.normal(rng_keys[0], act_shape, jnp.float32)
    row_tilt = jax.random.normal(rng_keys[1], (NUM_SEQS, SEQ_LEN, 1), jnp.float32)
    x = (base_noise + row_tilt * feat_ramp).astype(jnp.bfloat16)
    ln_g = 1.0 + 0.5 * jax.random.normal(rng_keys[2], (HIDDEN,), jnp.float32)
    ln_b = 0.5 * jax.random.normal(rng_keys[3], (HIDDEN,), jnp.float32)
    fan_scale = HIDDEN ** -0.5
    qkv_shift = jax.random.normal(rng_keys[4], (3 * HIDDEN,), jnp.float32)
    qkv_noise = jax.random.normal(rng_keys[5], (HIDDEN, 3 * HIDDEN), jnp.float32)
    w_qkv = ((qkv_noise + qkv_shift) * fan_scale).astype(jnp.bfloat16)
    b_qkv = 0.5 * jax.random.normal(rng_keys[6], (3 * NUM_HEADS, HEAD_DIM), jnp.float32)
    w_o = (jax.random.normal(rng_keys[7], (HIDDEN, HIDDEN), jnp.float32) * fan_scale).astype(jnp.bfloat16)
    b_o = 0.5 * jax.random.normal(rng_keys[8], (HIDDEN,), jnp.float32)
    d_y = jax.random.normal(rng_keys[9], act_shape, jnp.float32).astype(jnp.bfloat16)
    return {"x": x, "ln_g": ln_g, "ln_b": ln_b, "w_qkv": w_qkv, "b_qkv": b_qkv, "w_o": w_o, "b_o": b_o, "d_y": d_y}


def snap_bf16(arr_in):
    return arr_in + lax.stop_gradient(arr_in.astype(jnp.bfloat16).astype(jnp.float32) - arr_in)


def block_forward(x_seq, ln_g, ln_b, w_qkv, b_qkv, w_o, b_o):
    row_mean = jnp.mean(x_seq, axis=-1, keepdims=True)
    centred = x_seq - row_mean
    row_var = jnp.mean(centred * centred, axis=-1, keepdims=True)
    x_norm = snap_bf16(centred * lax.rsqrt(row_var + LN_EPS) * ln_g + ln_b)
    qkv_vals = snap_bf16(jnp.dot(x_norm, w_qkv, preferred_element_type=jnp.float32) + b_qkv.reshape(-1))
    qkv_vals = qkv_vals.reshape(SEQ_LEN, COL_BLOCKS, 3, HEADS_PER_COL, HEAD_DIM)
    q_rows = qkv_vals[:, :, 0].reshape(SEQ_LEN, NUM_HEADS, HEAD_DIM)
    k_rows = qkv_vals[:, :, 1].reshape(SEQ_LEN, NUM_HEADS, HEAD_DIM)
    v_rows = qkv_vals[:, :, 2].reshape(SEQ_LEN, NUM_HEADS, HEAD_DIM)
    scores = jnp.einsum("qnd,knd->nqk", q_rows, k_rows) * HEAD_DIM ** -0.5
    positions = jnp.arange(SEQ_LEN)
    causal = positions[:, None] >= positions[None, :]
    scores = jnp.where(causal, scores, -1e30)
    prob_vals = snap_bf16(jax.nn.softmax(scores, axis=-1))
    att_vals = snap_bf16(jnp.einsum("nqk,knd->qnd", prob_vals, v_rows)).reshape(SEQ_LEN, HIDDEN)
    out_proj = jnp.dot(att_vals, w_o, preferred_element_type=jnp.float32) + b_o
    return snap_bf16(x_seq + out_proj)


def reference(x, ln_g, ln_b, w_qkv, b_qkv, w_o, b_o, d_y):
    w_qkv_f = w_qkv.astype(jnp.float32)
    w_o_f = w_o.astype(jnp.float32)
    grad_zero = (jnp.zeros_like(ln_g), jnp.zeros_like(ln_b), jnp.zeros_like(w_qkv_f), jnp.zeros_like(b_qkv), jnp.zeros_like(w_o_f), jnp.zeros_like(b_o))

    def seq_step(grad_acc, seq_pair):
        x_seq, dy_seq = seq_pair
        y_seq, pull_back = jax.vjp(block_forward, x_seq.astype(jnp.float32), ln_g, ln_b, w_qkv_f, b_qkv, w_o_f, b_o)
        seq_grads = pull_back(dy_seq.astype(jnp.float32))
        grad_acc = tuple(acc_old + new_grad for acc_old, new_grad in zip(grad_acc, seq_grads[1:]))
        return grad_acc, (y_seq.astype(jnp.bfloat16), seq_grads[0].astype(jnp.bfloat16))

    grad_sums, outs_seq = lax.scan(seq_step, grad_zero, (x, d_y))
    y_out, d_x = outs_seq
    dln_g, dln_b, dw_qkv, db_qkv, dw_o, db_o = grad_sums
    return (y_out, d_x, dw_qkv.astype(jnp.bfloat16), db_qkv, dw_o.astype(jnp.bfloat16), db_o, dln_g, dln_b)
```

```python
import functools

import jax
import jax.numpy as jnp
from jax import lax
from jax.experimental import pallas as pl
from jax.experimental.pallas import tpu as pltpu
from jax.sharding import PartitionSpec as P


LN_EPS = 1e-5
SWAP = [(0, 1), (1, 0)]
F32 = jnp.float32
BF16 = jnp.bfloat16
LOG2E = 1.4426950408889634


def nt_dot(lhs, rhs):
    return lax.dot_general(lhs, rhs, (((1,), (1,)), ((), ())), preferred_element_type=F32)


def tn_dot(lhs, rhs):
    return lax.dot_general(lhs, rhs, (((0,), (0,)), ((), ())), preferred_element_type=F32)


def nn_dot(lhs, rhs):
    return lax.dot_general(lhs, rhs, (((1,), (0,)), ((), ())), preferred_element_type=F32)


def row_sum(val):
    return jnp.sum(val, -1, keepdims=True)


def group_rows(i, unroll, step):
    return [pl.ds(pl.multiple_of((i * unroll + u) * step, step), step) for u in range(unroll)]


def ln_fwd_body(col_ref, own_ref, recv_ref, g_ref, b_ref, *rest):
    xn_ref = rest[-1]
    width = own_ref.shape[1]
    inv_n = 1.0 / (2 * width)
    col = col_ref[0]
    own_cols = pl.ds(pl.multiple_of(col * width, width), width)
    far_cols = pl.ds(pl.multiple_of((1 - col) * width, width), width)
    step, unroll = 16, 4

    @pl.loop(0, own_ref.shape[0] // (step * unroll))
    def _(i):
        groups = group_rows(i, unroll, step)
        means = [row_sum(own_ref[r, :].astype(F32) + recv_ref[r, :].astype(F32)) * inv_n for r in groups]
        invs = []
        for r, mean in zip(groups, means):
            own = own_ref[r, :].astype(F32) - mean
            far = recv_ref[r, :].astype(F32) - mean
            invs.append(lax.rsqrt(row_sum(own * own + far * far) * inv_n + LN_EPS))
        for r, mean, inv in zip(groups, means, invs):
            for src, cols in ((own_ref, own_cols), (recv_ref, far_cols)):
                hat = (src[r, :].astype(F32) - mean) * inv
                xn_ref[r, cols] = (hat * g_ref[:, cols] + b_ref[:, cols]).astype(BF16)


def ln_fwd(col, x_loc, x_recv, g_full, b_full, row0, total, prev):
    rows, width = x_recv.shape
    blk = 256
    nall = total // blk
    off = row0 // blk
    in_specs = [
        pl.BlockSpec((blk, width), lambda i, c: (i + off + c[0] * nall, 0)),
        pl.BlockSpec((blk, width), lambda i, c: (i, 0)),
        pl.BlockSpec((1, 2 * width), lambda i, c: (0, 0)),
        pl.BlockSpec((1, 2 * width), lambda i, c: (0, 0)),
    ]
    args = [col, x_loc, x_recv, g_full, b_full]
    aliases = {}
    if prev is not None:
        in_specs.append(pl.BlockSpec(memory_space=pl.ANY))
        args.append(prev)
        aliases = {5: 0}
    return pl.pallas_call(
        ln_fwd_body,
        out_shape=jax.ShapeDtypeStruct((total, 2 * width), BF16),
        grid_spec=pltpu.PrefetchScalarGridSpec(
            num_scalar_prefetch=1,
            grid=(rows // blk,),
            in_specs=in_specs,
            out_specs=pl.BlockSpec((blk, 2 * width), lambda i, c: (i + off, 0)),
        ),
        input_output_aliases=aliases,
        cost_estimate=pl.CostEstimate(flops=20 * rows * 2 * width, bytes_accessed=8 * rows * width, transcendentals=0),
        name="ln_fwd",
    )(*args)


def ln_bwd_body(col_ref, dxn_ref, own_ref, recv_ref, dy_own_ref, dy_recv_ref, g_ref, *rest):
    dx_own_ref, dx_send_ref, dg_ref, db_ref = rest[-4:]
    width = own_ref.shape[1]
    inv_n = 1.0 / (2 * width)
    col = col_ref[0]
    own_cols = pl.ds(pl.multiple_of(col * width, width), width)
    far_cols = pl.ds(pl.multiple_of((1 - col) * width, width), width)
    step, unroll = 16, 8

    @pl.when(pl.program_id(0) == 0)
    def _():
        dg_ref[...] = jnp.zeros_like(dg_ref)
        db_ref[...] = jnp.zeros_like(db_ref)

    def fold(val):
        return jnp.sum(val.reshape(val.shape[0] // 8, 8, val.shape[1]), axis=0)

    @pl.loop(0, own_ref.shape[0] // (step * unroll))
    def _(i):
        groups = group_rows(i, unroll, step)
        stats = []
        for r in groups:
            mean = row_sum(own_ref[r, :].astype(F32) + recv_ref[r, :].astype(F32)) * inv_n
            m1 = row_sum(dxn_ref[r, own_cols] * g_ref[:, own_cols] + dxn_ref[r, far_cols] * g_ref[:, far_cols]) * inv_n
            stats.append((mean, m1))
        full = []
        for r, (mean, m1) in zip(groups, stats):
            own = own_ref[r, :].astype(F32) - mean
            far = recv_ref[r, :].astype(F32) - mean
            var = row_sum(own * own + far * far) * inv_n
            m2 = row_sum(dxn_ref[r, own_cols] * g_ref[:, own_cols] * own + dxn_ref[r, far_cols] * g_ref[:, far_cols] * far) * inv_n
            inv = lax.rsqrt(var + LN_EPS)
            full.append((mean, inv, m1, m2 * inv))
        for src, dy, dx, cols in ((own_ref, dy_own_ref, dx_own_ref, own_cols), (recv_ref, dy_recv_ref, dx_send_ref, far_cols)):
            sum_g = sum_b = None
            for r, (mean, inv, m1, m2) in zip(groups, full):
                hat = (src[r, :].astype(F32) - mean) * inv
                d = dxn_ref[r, cols]
                add_g, add_b = fold(d * hat), fold(d)
                sum_g = add_g if sum_g is None else sum_g + add_g
                sum_b = add_b if sum_b is None else sum_b + add_b
                dx[r, :] = (dy[r, :].astype(F32) + inv * (d * g_ref[:, cols] - m1 - hat * m2)).astype(BF16)
            dg_ref[:, cols] += sum_g
            db_ref[:, cols] += sum_b


def ln_bwd(col, dxn, x_loc, x_recv, dy_loc, dy_recv, g_full, row0, total, dx_prev):
    rows, width = dxn.shape[0], dy_recv.shape[1]
    blk = 128
    nall = total // blk
    nblk = rows // blk
    off = row0 // blk
    own_spec = pl.BlockSpec((blk, width), lambda i, c: (i + off + c[0] * nall, 0))
    recv_spec = pl.BlockSpec((blk, width), lambda i, c: (i + off, 0))
    npiece = x_recv[0].shape[0] // blk
    x_specs = [pl.BlockSpec((blk, width), lambda i, c, p=p: (jnp.clip(i + off - p * npiece, 0, npiece - 1), 0)) for p in range(2)]
    in_specs = [
        pl.BlockSpec((blk, 2 * width), lambda i, c: (i, 0)),
        own_spec,
        *x_specs,
        own_spec,
        recv_spec,
        pl.BlockSpec((1, 2 * width), lambda i, c: (0, 0)),
    ]
    args = [col, dxn, x_loc, *x_recv, dy_loc, dy_recv, g_full]
    aliases = {}
    if dx_prev is not None:
        in_specs.append(pl.BlockSpec(memory_space=pl.ANY))
        args.append(dx_prev)
        aliases = {8: 0}

    def body(col_ref, dxn_ref, own_ref, x0_ref, x1_ref, *rest):
        late = pl.program_id(0) + off >= npiece

        @pl.when(jnp.logical_not(late))
        def _():
            ln_bwd_body(col_ref, dxn_ref, own_ref, x0_ref, *rest)

        @pl.when(late)
        def _():
            ln_bwd_body(col_ref, dxn_ref, own_ref, x1_ref, *rest)

    return pl.pallas_call(
        body,
        out_shape=(
            jax.ShapeDtypeStruct((2 * total, width), BF16),
            jax.ShapeDtypeStruct((rows, width), BF16),
            jax.ShapeDtypeStruct((8, 2 * width), F32),
            jax.ShapeDtypeStruct((8, 2 * width), F32),
        ),
        grid_spec=pltpu.PrefetchScalarGridSpec(
            num_scalar_prefetch=1,
            grid=(nblk,),
            in_specs=in_specs,
            out_specs=(
                own_spec,
                pl.BlockSpec((blk, width), lambda i, c: (i, 0)),
                pl.BlockSpec((8, 2 * width), lambda i, c: (0, 0)),
                pl.BlockSpec((8, 2 * width), lambda i, c: (0, 0)),
            ),
        ),
        input_output_aliases=aliases,
        cost_estimate=pl.CostEstimate(flops=40 * rows * 2 * width, bytes_accessed=20 * rows * width, transcendentals=0),
        name="ln_bwd",
    )(*args)


def attn_fwd_body(heads, scale, grp_ref, q_ref, k_ref, v_ref, *rest):
    out_ref = rest[-1]
    half = q_ref.shape[0] // 2
    causal = lax.broadcasted_iota(jnp.int32, (half, half), 0) >= lax.broadcasted_iota(jnp.int32, (half, half), 1)
    unroll = 8
    coef = scale * LOG2E

    @pl.loop(0, heads // unroll)
    def _(i):
        scores = []
        for j in range(unroll):
            cols = pl.ds(pl.multiple_of((i * unroll + j) * 128, 128), 128)
            k = k_ref[:, cols]
            scores.append((cols, nt_dot(q_ref[:half, cols], k[:half]), nt_dot(q_ref[half:, cols], k)))
        probs = []
        for cols, s0, s1 in scores:
            sa = jnp.where(causal, s0, -1e30)
            ea = jnp.exp2((sa - jnp.max(sa, -1, keepdims=True)) * coef)
            pa = (ea * (1.0 / row_sum(ea))).astype(BF16)
            sb, sc = s1[:, :half], jnp.where(causal, s1[:, half:], -1e30)
            top = jnp.max(jnp.maximum(sb, sc), -1, keepdims=True)
            eb, ec = jnp.exp2((sb - top) * coef), jnp.exp2((sc - top) * coef)
            inv = 1.0 / row_sum(eb + ec)
            probs.append((cols, pa, jnp.concatenate([(eb * inv).astype(BF16), (ec * inv).astype(BF16)], axis=1)))
        for cols, p0, p1 in probs:
            v = v_ref[:, cols]
            out_ref[:half, cols] = nn_dot(p0, v[:half]).astype(BF16)
            out_ref[half:, cols] = nn_dot(p1, v).astype(BF16)


def attn_fwd(grp, qkv, groups, width, seq, row0, total, prev):
    rows = qkv.shape[0]
    heads = width // 128
    off = row0 // seq
    in_specs = [pl.BlockSpec((seq, width), lambda g, i, c, j=j: (i, 3 * g + j)) for j in range(3)]
    args = [grp, qkv, qkv, qkv]
    aliases = {}
    if prev is not None:
        in_specs.append(pl.BlockSpec(memory_space=pl.ANY))
        args.append(prev)
        aliases = {4: 0}
    nheads = rows // seq * heads * groups
    return pl.pallas_call(
        functools.partial(attn_fwd_body, heads, 128 ** -0.5),
        out_shape=jax.ShapeDtypeStruct((total, 4096), BF16),
        grid_spec=pltpu.PrefetchScalarGridSpec(
            num_scalar_prefetch=1,
            grid=(groups, rows // seq),
            in_specs=in_specs,
            out_specs=pl.BlockSpec((seq, width), lambda g, i, c: (i + off, c[0] + g)),
        ),
        input_output_aliases=aliases,
        cost_estimate=pl.CostEstimate(flops=nheads * seq * seq * 128 * 8, bytes_accessed=8 * rows * width * groups, transcendentals=nheads * seq * seq),
        name="attn_fwd",
    )(*args)


def attn_bwd_body(heads, scale, grp_ref, q_ref, k_ref, v_ref, d_ref, *rest):
    dq_ref, sum_ref = rest[-2:]
    seq, width = q_ref.shape
    half = seq // 2
    causal = lax.broadcasted_iota(jnp.int32, (half, half), 1) >= lax.broadcasted_iota(jnp.int32, (half, half), 0)
    unroll = 8
    coef = scale * LOG2E

    @pl.when(pl.program_id(0) == 0)
    def _():
        sum_ref[...] = jnp.zeros_like(sum_ref)

    def col_sum(val):
        return jnp.sum(val, 0, keepdims=True)

    def emit(top, bottom, start):
        cols = pl.ds(pl.multiple_of(start, 128), 128)
        dq_ref[:half, cols] = top.astype(BF16)
        dq_ref[half:, cols] = bottom.astype(BF16)
        sum_ref[:, cols] += jnp.sum((top + bottom).reshape(half // 8, 8, 128), axis=0)

    @pl.loop(0, heads // unroll)
    def _(i):
        first = []
        for j in range(unroll):
            h = (i * unroll + j) * 128
            cols = pl.ds(pl.multiple_of(h, 128), 128)
            q, k, v, d = q_ref[:, cols], k_ref[:, cols], v_ref[:, cols], d_ref[:, cols]
            first.append((h, cols, nt_dot(k[:half], q), nt_dot(k[half:], q[half:]), nt_dot(v[:half], d), nt_dot(v[half:], d[half:])))
        second = []
        for h, cols, s0, s1, dp0, dpc in first:
            sa = jnp.where(causal, s0[:, :half], -1e30)
            ea = jnp.exp2((sa - jnp.max(sa, 0, keepdims=True)) * coef)
            pa = ea * (1.0 / col_sum(ea))
            dpa, dpb = dp0[:, :half], dp0[:, half:]
            dsa = (pa * (dpa - col_sum(dpa * pa)) * scale).astype(BF16)
            sb, sc = s0[:, half:], jnp.where(causal, s1, -1e30)
            top = jnp.max(jnp.maximum(sb, sc), 0, keepdims=True)
            eb, ec = jnp.exp2((sb - top) * coef), jnp.exp2((sc - top) * coef)
            inv = 1.0 / col_sum(eb + ec)
            pb, pc = eb * inv, ec * inv
            dot = col_sum(dpb * pb + dpc * pc)
            dsb = (pb * (dpb - dot) * scale).astype(BF16)
            dsc = (pc * (dpc - dot) * scale).astype(BF16)
            p0 = jnp.concatenate([pa.astype(BF16), pb.astype(BF16)], axis=1)
            second.append((h, cols, p0, pc.astype(BF16), dsa, dsb, dsc))
        for h, cols, p0, p1, dsa, dsb, dsc in second:
            q, k, d = q_ref[:, cols], k_ref[:, cols], d_ref[:, cols]
            emit(nn_dot(p0, d), nn_dot(p1, d[half:]), h + 2 * width)
            emit(nn_dot(jnp.concatenate([dsa, dsb], axis=1), q), nn_dot(dsc, q[half:]), h + width)
            emit(tn_dot(dsa, k[:half]), tn_dot(jnp.concatenate([dsb, dsc], axis=0), k), h)


def attn_bwd(grp, qkv, d_att, group, out_groups, width, seq, row0, total, prev):
    rows = qkv.shape[0]
    heads = width // 128
    off = row0 // seq
    in_specs = [pl.BlockSpec((seq, width), lambda i, c, j=j: (i, 3 * group + j)) for j in range(3)]
    in_specs.append(pl.BlockSpec((seq, width), lambda i, c: (i + off, c[0])))
    args = [grp, qkv, qkv, qkv, d_att]
    aliases = {}
    if prev is not None:
        in_specs.append(pl.BlockSpec(memory_space=pl.ANY))
        args.append(prev)
        aliases = {5: 0}
    nheads = rows // seq * heads
    return pl.pallas_call(
        functools.partial(attn_bwd_body, heads, 128 ** -0.5),
        out_shape=(
            jax.ShapeDtypeStruct((total, 3 * width * out_groups), BF16),
            jax.ShapeDtypeStruct((8, 3 * width), F32),
        ),
        grid_spec=pltpu.PrefetchScalarGridSpec(
            num_scalar_prefetch=1,
            grid=(rows // seq,),
            in_specs=in_specs,
            out_specs=(
                pl.BlockSpec((seq, 3 * width), lambda i, c: (i + off, group)),
                pl.BlockSpec((8, 3 * width), lambda i, c: (0, 0)),
            ),
        ),
        input_output_aliases=aliases,
        cost_estimate=pl.CostEstimate(flops=nheads * seq * seq * 128 * 20, bytes_accessed=14 * rows * width, transcendentals=nheads * seq * seq),
        name="attn_bwd",
    )(*args)


def assemble_body(pos_ref, own_ref, recv_ref, out_ref):
    half = pl.num_programs(0) // 2
    mine = (pl.program_id(0) // half) == pos_ref[0]

    @pl.when(mine)
    def _():
        out_ref[...] = own_ref[...]

    @pl.when(jnp.logical_not(mine))
    def _():
        out_ref[...] = recv_ref[...]


def assemble(pos, own, recv, blk):
    rows, width = own.shape
    half = rows // blk

    def own_map(i, p):
        return (jnp.clip(i - p[0] * half, 0, half - 1), 0)

    def recv_map(i, p):
        return (jnp.clip(i - (1 - p[0]) * half, 0, half - 1), 0)

    return pl.pallas_call(
        assemble_body,
        out_shape=jax.ShapeDtypeStruct((2 * rows, width), own.dtype),
        grid_spec=pltpu.PrefetchScalarGridSpec(
            num_scalar_prefetch=1,
            grid=(2 * half,),
            in_specs=[pl.BlockSpec((blk, width), own_map), pl.BlockSpec((blk, width), recv_map)],
            out_specs=pl.BlockSpec((blk, width), lambda i, p: (i, 0)),
        ),
        cost_estimate=pl.CostEstimate(flops=rows * width, bytes_accessed=8 * rows * width, transcendentals=0),
        name="assemble",
    )(pos, own, recv)


def regroup_body(src_ref, out_ref):
    wide = src_ref.shape[1] // 6
    for j in range(2):
        for t in range(3):
            out_ref[:, (3 * j + t) * wide:(3 * j + t + 1) * wide] = src_ref[:, (2 * t + j) * wide:(2 * t + j + 1) * wide]


def regroup(val):
    rows, width = val.shape
    spec = pl.BlockSpec((256, width), lambda i: (i, 0))
    return pl.pallas_call(
        regroup_body,
        out_shape=jax.ShapeDtypeStruct(val.shape, val.dtype),
        grid=(rows // 256,),
        in_specs=[spec],
        out_specs=spec,
        cost_estimate=pl.CostEstimate(flops=rows * width, bytes_accessed=4 * rows * width, transcendentals=0),
        name="regroup",
    )(val)


def join_body(pos_ref, own_ref, recv_ref, half_ref, rest_ref, out_ref):
    wide = own_ref.shape[1] // 3
    steps = pl.num_programs(0) // 2
    mine = (pl.program_id(0) // steps) == pos_ref[0]

    def cols(t, j):
        return pl.ds((2 * t + j) * wide, wide)

    for src, flag in ((own_ref, mine), (recv_ref, jnp.logical_not(mine))):
        @pl.when(flag)
        def _(src=src):
            for t in range(3):
                out_ref[:, cols(t, 0)] = src[:, t * wide:(t + 1) * wide]

    for t in range(3):
        part = pl.ds(t * wide, wide)
        out_ref[:, cols(t, 1)] = (half_ref[:, part].astype(F32) + rest_ref[:, part].astype(F32)).astype(BF16)


def join(pos, own, recv, half, rest):
    rows, width = own.shape
    blk = 128
    steps = rows // blk
    own_spec = pl.BlockSpec((blk, width), lambda i, p: (jnp.clip(i - p[0] * steps, 0, steps - 1), 0))
    recv_spec = pl.BlockSpec((blk, width), lambda i, p: (jnp.clip(i - (1 - p[0]) * steps, 0, steps - 1), 0))
    full_spec = pl.BlockSpec((blk, width), lambda i, p: (i, 0))
    return pl.pallas_call(
        join_body,
        out_shape=jax.ShapeDtypeStruct((2 * rows, 2 * width), BF16),
        grid_spec=pltpu.PrefetchScalarGridSpec(
            num_scalar_prefetch=1,
            grid=(2 * steps,),
            in_specs=[own_spec, recv_spec, full_spec, full_spec],
            out_specs=pl.BlockSpec((blk, 2 * width), lambda i, p: (i, 0)),
        ),
        cost_estimate=pl.CostEstimate(flops=rows * width, bytes_accessed=20 * rows * width, transcendentals=0),
        name="join",
    )(pos, own, recv, half, rest)


def solution(mesh):
    act_spec = P(("depth", "row"), None, "col")
    mat_spec = P("row", "col")
    vec_spec = P("col")
    bias_spec = P("col", None)

    def swap(val, axis):
        return lax.ppermute(val, axis, SWAP)

    def tie(val, *deps):
        return lax.optimization_barrier((val,) + deps)[0]

    def gather(val, axes):
        return lax.all_gather(val, axes, axis=0, tiled=True)

    def scatter(val, axes):
        return lax.psum_scatter(val, axes, scatter_dimension=0, tiled=True)

    def block(x, ln_g, ln_b, w_qkv, b_qkv, w_o, b_o, d_y):
        num_seq, seq, width = x.shape
        half = num_seq // 2 * seq
        tokens = num_seq * seq
        piece = w_qkv.shape[0] // 2
        hw = width // 2
        col = lax.axis_index("col")
        dep = lax.axis_index("depth")
        other = 1 - col

        def grp_s(val):
            return jnp.reshape(val, (1,)).astype(jnp.int32)

        x2 = x.reshape(tokens, width)
        dy2 = d_y.reshape(tokens, width)
        col_arr, oth_arr, dep_arr = grp_s(col), grp_s(other), grp_s(dep)
        own_grp = [grp_s(col * 2 + j) for j in range(2)]
        oth_grp = [grp_s(other * 2 + j) for j in range(2)]

        def group_cols(val, j):
            return [val[:, t * width + j * hw:t * width + (j + 1) * hw] for t in range(3)]

        def slab(j):
            part = lax.dynamic_slice_in_dim(w_qkv, dep * piece, piece, 0)
            return jnp.concatenate(group_cols(part, j), axis=1)

        def send(val, axis="col"):
            return swap(val, axis)

        nb = hw // 128
        bias = jnp.concatenate([b_qkv[(2 * t + j) * nb:(2 * t + j + 1) * nb] for j in range(2) for t in range(3)], axis=0)
        vecs = jnp.concatenate([ln_g.reshape(-1, 128), ln_b.reshape(-1, 128), b_o.reshape(-1, 128), bias], axis=0)
        vecs_r = send(vecs)
        rows2 = half // 2
        x_out = [lax.dynamic_slice_in_dim(x2, other * half, rows2, 0)]
        slab_a = tie(slab(0), x_out[0])
        x_out.append(lax.dynamic_slice_in_dim(tie(x2, slab_a), other * half + rows2, rows2, 0))
        slab_b = tie(slab(1), x_out[1])
        wo_out = lax.dynamic_slice_in_dim(tie(w_o, slab_b), dep * piece, piece, 0)
        dy_out = lax.dynamic_slice_in_dim(tie(dy2, wo_out), other * half, half, 0)
        x_recv = [send(x_out[0])]
        wa_in = send(slab_a)
        x_recv.append(send(x_out[1]))
        wb_in = send(slab_b)
        wo_in = send(wo_out)
        dy_recv = send(dy_out)
        w_perm = regroup(tie(w_qkv, dy_out))
        wo_own = gather(w_o, "row")
        w_own = gather(w_perm, "row")

        nv = width // 128
        first = col == 0

        def both(lo, hi):
            a = vecs[lo:hi].reshape(1, -1)
            b = vecs_r[lo:hi].reshape(1, -1)
            return jnp.concatenate([jnp.where(first, a, b), jnp.where(first, b, a)], axis=1)

        g_full = both(0, nv)
        b_full = both(nv, 2 * nv)
        bo_oth = vecs_r[2 * nv:3 * nv].reshape(-1)
        bq_own = bias.reshape(-1)
        bq_oth = vecs_r[3 * nv:].reshape(2, 3 * hw)
        db_o = jnp.sum(dy2.astype(F32), axis=0)
        wq_oth = [None, None]
        qkv_oth = [None, None]
        dqkv_oth = [None, None]
        sum_oth = [None, None]

        def held(*vals):
            return lax.optimization_barrier(vals)

        def project(j):
            return (nn_dot(xn, wq_oth[j]) + bq_oth[j]).astype(BF16)

        def weight_grad(lhs, rhs):
            return tn_dot(lhs, rhs).astype(BF16)

        dy_own = lax.dynamic_slice_in_dim(tie(dy2, dy_out), col * half, half, 0)
        datt_part = nt_dot(tie(dy_own, w_perm), wo_own)

        xn = ln_fwd(col_arr, tie(x2, datt_part), x_recv[0], g_full, b_full, 0, half, None)
        qkv_own = [(nn_dot(xn[:rows2], w_own) + bq_own).astype(BF16)]
        wa_in, xn, qkv_own[0] = held(wa_in, xn, qkv_own[0])
        wq_oth[0] = gather(wa_in, ("row", "depth"))
        xn = ln_fwd(col_arr, x2, x_recv[1], g_full, b_full, rows2, half, xn)
        qkv_own.append((nn_dot(xn[rows2:], w_own) + bq_own).astype(BF16))
        att = None
        for i in range(2):
            att = attn_fwd(own_grp[0], qkv_own[i] if i else tie(qkv_own[0], qkv_own[1]), 2, hw, seq, i * rows2, half, att)
        wb_in, xn, att = held(wb_in, xn, att)
        wq_oth[1] = gather(wb_in, ("row", "depth"))
        qkv_oth[0] = project(0)
        att = attn_fwd(oth_grp[0], qkv_oth[0], 1, hw, seq, 0, half, att)
        wo_in, att, xn = held(wo_in, att, xn)
        wo_oth = gather(wo_in, ("row", "depth"))
        qkv_oth[1] = project(1)
        att = attn_fwd(oth_grp[1], qkv_oth[1], 1, hw, seq, 0, half, att)
        x_all = jnp.concatenate(x_recv, axis=0)
        y_send = (x_all.astype(F32) + nn_dot(att, wo_oth) + bo_oth).astype(BF16)
        y_recv = send(y_send)
        x_own = lax.dynamic_slice_in_dim(tie(x2, y_send), col * half, half, 0)
        y_own = (x_own.astype(F32) + nn_dot(att, wo_own) + b_o).astype(BF16)

        def back_far(j, gate):
            dqkv_oth[j], sum_oth[j] = attn_bwd(oth_grp[j], tie(qkv_oth[j], gate), d_att, 0, 1, hw, seq, 0, half, None)

        def back_own(j, gate, prev):
            total = 0.0
            for i in range(2):
                prev, part = attn_bwd(own_grp[j], tie(qkv_own[i], gate), d_att, j, 2, hw, seq, i * rows2, half, prev)
                total = total + part
            return prev, total

        wide = 3 * hw
        sum_own = [None, None]
        d_att = (nt_dot(tie(dy_recv, y_own), wo_oth) + datt_part).astype(BF16)
        dwo_far = weight_grad(tie(att, d_att), dy_recv)
        red_of = scatter(dwo_far, "row")
        back_far(0, dwo_far)
        dw_a = weight_grad(xn, dqkv_oth[0])
        red_a = scatter(dw_a, ("row", "depth"))
        red_of, dw_a = held(red_of, dw_a)
        far_o = send(red_of)
        dwo_near = weight_grad(tie(att, dw_a), dy_own)
        red_on = scatter(dwo_near, "row")
        back_far(1, dwo_near)
        dw_b = weight_grad(xn, dqkv_oth[1])
        red_b = scatter(dw_b, "row")
        far_o, red_on, red_a, dw_b = held(far_o, red_on, red_a, dw_b)
        far_a = send(red_a)
        half_o = (red_on.astype(F32) + far_o.astype(F32)).astype(BF16)
        half_r = send(half_o, "depth")
        dqkv_own, sum_own[0] = back_own(0, half_o, None)
        dw_oa = weight_grad(xn, dqkv_own[:, :wide])
        red_oa = scatter(dw_oa, ("row", "depth"))
        red_b, dw_oa = held(red_b, dw_oa)
        far_b = send(red_b)
        dqkv_own, sum_own[1] = back_own(1, dw_oa, dqkv_own)
        dw_ob = weight_grad(xn, dqkv_own[:, wide:])
        red_ob = scatter(dw_ob, "row")

        parts = (half // 3,) * 3
        dx, gate = None, dw_ob
        dx_recv, sums_n = [], []
        for part in range(len(parts)):
            lo, rows = part * parts[0], parts[part]
            dxn = nt_dot(tie(dqkv_own, gate)[lo:lo + rows], w_own)
            if part == 0:
                far_a, red_oa, dxn = held(far_a, red_oa, dxn)
                half_a = (red_oa.astype(F32) + far_a.astype(F32)).astype(BF16)
                rest_a = send(half_a, "depth")
                dxn = tie(dxn, half_a)
            dxn = nt_dot(dqkv_oth[0][lo:lo + rows], wq_oth[0]) + dxn
            if part == 0:
                far_b, red_ob, dxn = held(far_b, red_ob, dxn)
                half_b = (red_ob.astype(F32) + far_b.astype(F32)).astype(BF16)
                rest_b = send(half_b, "depth")
                dxn = tie(dxn, half_b)
            dxn = nt_dot(dqkv_oth[1][lo:lo + rows], wq_oth[1]) + dxn
            dx, dx_send, dg8, db8 = ln_bwd(col_arr, dxn, x2, x_recv, dy2, dy_recv, g_full, lo, half, dx)
            sums_n.append((dg8, db8))
            dx_recv.append(send(dx_send))
            gate = dx_send
        y = assemble(col_arr, y_own, tie(y_recv, gate), 256)
        dw_o = (tie(half_o, y).astype(F32) + half_r.astype(F32)).astype(BF16)
        dw_qkv = join(dep_arr, half_a, tie(rest_a, dw_o), half_b, rest_b)
        dg8 = sum(pair[0] for pair in sums_n)
        db8 = sum(pair[1] for pair in sums_n)

        def natural(pair):
            vals = [jnp.sum(s, axis=0).reshape(3, hw) for s in pair]
            return jnp.concatenate([vals[j][t] for t in range(3) for j in range(2)])

        dg = jnp.sum(dg8, axis=0)
        dbn = jnp.sum(db8, axis=0)
        far = jnp.concatenate([natural(sum_oth), lax.dynamic_slice_in_dim(dg, other * width, width), lax.dynamic_slice_in_dim(dbn, other * width, width)])
        near = jnp.concatenate([natural(sum_own), lax.dynamic_slice_in_dim(dg, col * width, width), lax.dynamic_slice_in_dim(dbn, col * width, width)])
        total = near.reshape(-1, 128) + send(far.reshape(-1, 128))
        total, db_o = lax.psum((total, db_o), ("depth", "row"))
        for part in range(len(parts)):
            dx = lax.dynamic_update_slice(dx, tie(dx_recv[part], dw_o if part < 2 else dw_qkv), (other * half + part * parts[0], 0))
        nq = 3 * nv
        return (
            y.reshape(x.shape),
            dx.reshape(x.shape),
            dw_qkv,
            total[:nq],
            dw_o,
            db_o,
            total[nq:nq + nv].reshape(-1),
            total[nq + nv:].reshape(-1),
        )

    return jax.shard_map(
        block,
        mesh=mesh,
        in_specs=(act_spec, vec_spec, vec_spec, mat_spec, bias_spec, mat_spec, vec_spec, act_spec),
        out_specs=(act_spec, act_spec, mat_spec, bias_spec, mat_spec, vec_spec, vec_spec, vec_spec),
        check_vma=False,
    )
```

```python
import functools

import jax
import jax.numpy as jnp
from jax import lax
from jax.experimental import pallas as pl
from jax.experimental.pallas import tpu as pltpu
from jax.sharding import PartitionSpec as P


LN_EPS = 1e-5
SWAP = [(0, 1), (1, 0)]
F32 = jnp.float32
BF16 = jnp.bfloat16
LOG2E = 1.4426950408889634


def nt_dot(lhs, rhs):
    return lax.dot_general(lhs, rhs, (((1,), (1,)), ((), ())), preferred_element_type=F32)


def tn_dot(lhs, rhs):
    return lax.dot_general(lhs, rhs, (((0,), (0,)), ((), ())), preferred_element_type=F32)


def nn_dot(lhs, rhs):
    return lax.dot_general(lhs, rhs, (((1,), (0,)), ((), ())), preferred_element_type=F32)


def row_sum(val):
    return jnp.sum(val, -1, keepdims=True)


def group_rows(i, unroll, step):
    return [pl.ds(pl.multiple_of((i * unroll + u) * step, step), step) for u in range(unroll)]


def ln_fwd_body(col_ref, own_ref, recv_ref, g_ref, b_ref, *rest):
    xn_ref, stat_ref = rest[-2:]
    width = own_ref.shape[1]
    inv_n = 1.0 / (2 * width)
    col = col_ref[0]
    own_cols = pl.ds(pl.multiple_of(col * width, width), width)
    far_cols = pl.ds(pl.multiple_of((1 - col) * width, width), width)
    step, unroll = 16, 4

    @pl.loop(0, own_ref.shape[0] // (step * unroll))
    def _(i):
        groups = group_rows(i, unroll, step)
        means = [row_sum(own_ref[r, :].astype(F32) + recv_ref[r, :].astype(F32)) * inv_n for r in groups]
        invs = []
        for r, mean in zip(groups, means):
            own = own_ref[r, :].astype(F32) - mean
            far = recv_ref[r, :].astype(F32) - mean
            invs.append(lax.rsqrt(row_sum(own * own + far * far) * inv_n + LN_EPS))
        for r, mean, inv in zip(groups, means, invs):
            stat_ref[r, :128] = jnp.broadcast_to(mean, (step, 128))
            stat_ref[r, 128:] = jnp.broadcast_to(inv, (step, 128))
            for src, cols in ((own_ref, own_cols), (recv_ref, far_cols)):
                hat = (src[r, :].astype(F32) - mean) * inv
                xn_ref[r, cols] = (hat * g_ref[:, cols] + b_ref[:, cols]).astype(BF16)


def ln_fwd(col, x_loc, x_recv, g_full, b_full, row0, total, prev):
    rows, width = x_recv.shape
    blk = 256
    nall = total // blk
    off = row0 // blk
    in_specs = [
        pl.BlockSpec((blk, width), lambda i, c: (i + off + c[0] * nall, 0)),
        pl.BlockSpec((blk, width), lambda i, c: (i, 0)),
        pl.BlockSpec((1, 2 * width), lambda i, c: (0, 0)),
        pl.BlockSpec((1, 2 * width), lambda i, c: (0, 0)),
    ]
    args = [col, x_loc, x_recv, g_full, b_full]
    aliases = {}
    if prev is not None:
        in_specs.extend([pl.BlockSpec(memory_space=pl.ANY)] * 2)
        args.extend(prev)
        aliases = {5: 0, 6: 1}
    return pl.pallas_call(
        ln_fwd_body,
        out_shape=(jax.ShapeDtypeStruct((total, 2 * width), BF16), jax.ShapeDtypeStruct((total, 256), F32)),
        grid_spec=pltpu.PrefetchScalarGridSpec(
            num_scalar_prefetch=1,
            grid=(rows // blk,),
            in_specs=in_specs,
            out_specs=(pl.BlockSpec((blk, 2 * width), lambda i, c: (i + off, 0)), pl.BlockSpec((blk, 256), lambda i, c: (i + off, 0))),
        ),
        input_output_aliases=aliases,
        cost_estimate=pl.CostEstimate(flops=20 * rows * 2 * width, bytes_accessed=8 * rows * width, transcendentals=0),
        name="ln_fwd",
    )(*args)


def ln_bwd_rows(dxn_ref, sides, stat_ref, g_ref, dg_ref, db_ref):
    rows = dxn_ref.shape[0]
    inv_n = 1.0 / dxn_ref.shape[1]
    step, unroll = 16, 4

    def fold(val):
        return jnp.sum(val.reshape(val.shape[0] // 8, 8, val.shape[1]), axis=0)

    @pl.loop(0, rows // (step * unroll))
    def _(i):
        groups = group_rows(i, unroll, step)
        full = []
        for r in groups:
            mean, inv = stat_ref[r, 0:1], stat_ref[r, 128:129]
            m1, m2 = 0.0, 0.0
            for x_ref, _, _, cols in sides:
                part = dxn_ref[r, cols] * g_ref[:, cols]
                m1 = m1 + part
                m2 = m2 + part * (x_ref[r, :].astype(F32) - mean)
            full.append((mean, inv, row_sum(m1) * inv_n, row_sum(m2) * inv_n * inv))
        for x_ref, dy_ref, dx_ref, cols in sides:
            sum_g = sum_b = None
            for r, (mean, inv, m1, m2) in zip(groups, full):
                hat = (x_ref[r, :].astype(F32) - mean) * inv
                d = dxn_ref[r, cols]
                add_g, add_b = fold(d * hat), fold(d)
                sum_g = add_g if sum_g is None else sum_g + add_g
                sum_b = add_b if sum_b is None else sum_b + add_b
                dx_ref[r, :] = (dy_ref[r, :].astype(F32) + inv * (d * g_ref[:, cols] - m1 - hat * m2)).astype(BF16)
            dg_ref[:, cols] += sum_g
            db_ref[:, cols] += sum_b


def dx_body(row0, half, col_ref, d_own, d_a, d_b, w_own, w_a, w_b, x_ref, x0_ref, x1_ref, dy_ref, dyr_ref, stat_ref, g_ref, *rest):
    dx_ref, send_ref, dg_ref, db_ref, acc, w_buf, d_buf, ln_buf, sems, ln_sems = rest[-10:]
    m, steps = pl.program_id(0), pl.num_programs(0)
    blk, wide = d_buf.shape[1:]
    width = x_ref.shape[1]
    col = col_ref[0]
    sources, count = [], 0
    for d, w in ((d_own, w_own), (d_a, w_a), (d_b, w_b)):
        chunks = d.shape[1] // wide
        sources.append((d, w, count, chunks))
        count += chunks

    def copies(d, w, block, chunk, slot):
        rows = pl.ds(pl.multiple_of(row0 + block * blk, blk), blk)
        cols = pl.ds(pl.multiple_of(chunk * wide, wide), wide)
        return (
            pltpu.make_async_copy(w.at[:, cols], w_buf.at[slot], sems.at[0, slot]),
            pltpu.make_async_copy(d.at[rows, cols], d_buf.at[slot], sems.at[1, slot]),
        )

    def fetch(block, chunk, slot):
        for d, w, lo, chunks in sources:
            @pl.when((chunk >= lo) & (chunk < lo + chunks))
            def _():
                for copy in copies(d, w, block, chunk - lo, slot):
                    copy.start()

    @pl.when(m == 0)
    def _():
        dg_ref[...] = jnp.zeros_like(dg_ref)
        db_ref[...] = jnp.zeros_like(db_ref)
        fetch(0, 0, 0)

    row = row0 + m * blk
    own_rows = pl.ds(pl.multiple_of(col * half + row, blk), blk)
    far_rows = pl.ds(pl.multiple_of(row, blk), blk)
    pair = half // 2
    x0_rows = pl.ds(pl.multiple_of(jnp.minimum(row, pair - blk), blk), blk)
    x1_rows = pl.ds(pl.multiple_of(jnp.maximum(row - pair, 0), blk), blk)

    def ln_copy(i, src):
        return pltpu.make_async_copy(src, ln_buf.at[i], ln_sems.at[i])

    ln_copy(0, x_ref.at[own_rows]).start()
    ln_copy(2, dy_ref.at[own_rows]).start()
    ln_copy(3, dyr_ref.at[far_rows]).start()

    @pl.when(row < pair)
    def _():
        ln_copy(1, x0_ref.at[x0_rows]).start()

    @pl.when(row >= pair)
    def _():
        ln_copy(1, x1_ref.at[x1_rows]).start()

    acc[...] = jnp.zeros_like(acc)

    @pl.loop(0, count)
    def _(k):
        slot = lax.rem(m * count + k, 2)

        @pl.when(k + 1 < count)
        def _():
            fetch(m, k + 1, 1 - slot)

        @pl.when((k + 1 == count) & (m + 1 < steps))
        def _():
            fetch(m + 1, 0, 1 - slot)

        for copy in copies(d_a, w_a, 0, 0, slot):
            copy.wait()
        acc[...] += nt_dot(d_buf[slot], w_buf[slot])

    for i in range(4):
        ln_copy(i, dyr_ref.at[far_rows]).wait()
    own_cols = pl.ds(pl.multiple_of(col * width, width), width)
    far_cols = pl.ds(pl.multiple_of((1 - col) * width, width), width)
    sides = ((ln_buf.at[0], ln_buf.at[2], dx_ref, own_cols), (ln_buf.at[1], ln_buf.at[3], send_ref, far_cols))
    ln_bwd_rows(acc, sides, stat_ref, g_ref, dg_ref, db_ref)


def dx_part(col, dqkv, weights, x_loc, x_recv, dy_loc, dy_recv, stats, g_full, row0, rows, dx_prev):
    total, width = dy_recv.shape
    blk, wide = 512, 1024
    off = row0 // blk
    nall = total // blk
    own_spec = pl.BlockSpec((blk, width), lambda i, c: (i + off + c[0] * nall, 0))
    sums_spec = pl.BlockSpec((8, 2 * width), lambda i, c: (0, 0))
    any_spec = pl.BlockSpec(memory_space=pl.ANY)
    in_specs = [any_spec] * 11 + [pl.BlockSpec((blk, 256), lambda i, c: (i + off, 0)), pl.BlockSpec((1, 2 * width), lambda i, c: (0, 0))]
    args = [col, *dqkv, *weights, x_loc, *x_recv, dy_loc, dy_recv, stats, g_full]
    aliases = {}
    if dx_prev is not None:
        in_specs.append(any_spec)
        args.append(dx_prev)
        aliases = {14: 0}
    depth = sum(d.shape[1] for d in dqkv)
    return pl.pallas_call(
        functools.partial(dx_body, row0, total),
        out_shape=(
            jax.ShapeDtypeStruct((2 * total, width), BF16),
            jax.ShapeDtypeStruct((rows, width), BF16),
            jax.ShapeDtypeStruct((8, 2 * width), F32),
            jax.ShapeDtypeStruct((8, 2 * width), F32),
        ),
        grid_spec=pltpu.PrefetchScalarGridSpec(
            num_scalar_prefetch=1,
            grid=(rows // blk,),
            in_specs=in_specs,
            out_specs=(own_spec, pl.BlockSpec((blk, width), lambda i, c: (i, 0)), sums_spec, sums_spec),
            scratch_shapes=[
                pltpu.VMEM((blk, 2 * width), F32),
                pltpu.VMEM((2, 2 * width, wide), BF16),
                pltpu.VMEM((2, blk, wide), BF16),
                pltpu.VMEM((4, blk, width), BF16),
                pltpu.SemaphoreType.DMA((2, 2)),
                pltpu.SemaphoreType.DMA((4,)),
            ],
        ),
        input_output_aliases=aliases,
        compiler_params=pltpu.CompilerParams(vmem_limit_bytes=60 * 1024 * 1024),
        cost_estimate=pl.CostEstimate(flops=4 * rows * width * depth, bytes_accessed=(rows // blk) * 4 * width * depth, transcendentals=0),
        name="dx_part",
    )(*args)


def attn_fwd_body(heads, scale, grp_ref, q_ref, k_ref, v_ref, *rest):
    out_ref = rest[-1]
    half = q_ref.shape[0] // 2
    causal = lax.broadcasted_iota(jnp.int32, (half, half), 0) >= lax.broadcasted_iota(jnp.int32, (half, half), 1)
    unroll = 8
    coef = scale * LOG2E

    @pl.loop(0, heads // unroll)
    def _(i):
        scores = []
        for j in range(unroll):
            cols = pl.ds(pl.multiple_of((i * unroll + j) * 128, 128), 128)
            k = k_ref[:, cols]
            scores.append((cols, nt_dot(q_ref[:half, cols], k[:half]), nt_dot(q_ref[half:, cols], k)))
        probs = []
        for cols, s0, s1 in scores:
            sa = jnp.where(causal, s0, -1e30)
            ea = jnp.exp2((sa - jnp.max(sa, -1, keepdims=True)) * coef)
            pa = (ea * (1.0 / row_sum(ea))).astype(BF16)
            sb, sc = s1[:, :half], jnp.where(causal, s1[:, half:], -1e30)
            top = jnp.max(jnp.maximum(sb, sc), -1, keepdims=True)
            eb, ec = jnp.exp2((sb - top) * coef), jnp.exp2((sc - top) * coef)
            inv = 1.0 / row_sum(eb + ec)
            probs.append((cols, pa, jnp.concatenate([(eb * inv).astype(BF16), (ec * inv).astype(BF16)], axis=1)))
        for cols, p0, p1 in probs:
            v = v_ref[:, cols]
            out_ref[:half, cols] = nn_dot(p0, v[:half]).astype(BF16)
            out_ref[half:, cols] = nn_dot(p1, v).astype(BF16)


def attn_fwd(grp, qkv, groups, width, seq, row0, total, prev):
    rows = qkv.shape[0]
    heads = width // 128
    off = row0 // seq
    in_specs = [pl.BlockSpec((seq, width), lambda g, i, c, j=j: (i, 3 * g + j)) for j in range(3)]
    args = [grp, qkv, qkv, qkv]
    aliases = {}
    if prev is not None:
        in_specs.append(pl.BlockSpec(memory_space=pl.ANY))
        args.append(prev)
        aliases = {4: 0}
    nheads = rows // seq * heads * groups
    return pl.pallas_call(
        functools.partial(attn_fwd_body, heads, 128 ** -0.5),
        out_shape=jax.ShapeDtypeStruct((total, 4096), BF16),
        grid_spec=pltpu.PrefetchScalarGridSpec(
            num_scalar_prefetch=1,
            grid=(groups, rows // seq),
            in_specs=in_specs,
            out_specs=pl.BlockSpec((seq, width), lambda g, i, c: (i + off, c[0] + g)),
        ),
        input_output_aliases=aliases,
        cost_estimate=pl.CostEstimate(flops=nheads * seq * seq * 128 * 8, bytes_accessed=8 * rows * width * groups, transcendentals=nheads * seq * seq),
        name="attn_fwd",
    )(*args)


def attn_bwd_body(heads, scale, grp_ref, q_ref, k_ref, v_ref, d_ref, *rest):
    dq_ref, sum_ref = rest[-2:]
    seq, width = q_ref.shape
    half = seq // 2
    causal = lax.broadcasted_iota(jnp.int32, (half, half), 1) >= lax.broadcasted_iota(jnp.int32, (half, half), 0)
    unroll = 8
    coef = scale * LOG2E

    @pl.when(pl.program_id(0) == 0)
    def _():
        sum_ref[...] = jnp.zeros_like(sum_ref)

    def col_sum(val):
        return jnp.sum(val, 0, keepdims=True)

    def emit(top, bottom, start):
        cols = pl.ds(pl.multiple_of(start, 128), 128)
        dq_ref[:half, cols] = top.astype(BF16)
        dq_ref[half:, cols] = bottom.astype(BF16)
        sum_ref[:, cols] += jnp.sum((top + bottom).reshape(half // 8, 8, 128), axis=0)

    @pl.loop(0, heads // unroll)
    def _(i):
        first = []
        for j in range(unroll):
            h = (i * unroll + j) * 128
            cols = pl.ds(pl.multiple_of(h, 128), 128)
            q, k, v, d = q_ref[:, cols], k_ref[:, cols], v_ref[:, cols], d_ref[:, cols]
            first.append((h, cols, nt_dot(k[:half], q), nt_dot(k[half:], q[half:]), nt_dot(v[:half], d), nt_dot(v[half:], d[half:])))
        second = []
        for h, cols, s0, s1, dp0, dpc in first:
            sa = jnp.where(causal, s0[:, :half], -1e30)
            ea = jnp.exp2((sa - jnp.max(sa, 0, keepdims=True)) * coef)
            pa = ea * (1.0 / col_sum(ea))
            dpa, dpb = dp0[:, :half], dp0[:, half:]
            dsa = (pa * (dpa - col_sum(dpa * pa)) * scale).astype(BF16)
            sb, sc = s0[:, half:], jnp.where(causal, s1, -1e30)
            top = jnp.max(jnp.maximum(sb, sc), 0, keepdims=True)
            eb, ec = jnp.exp2((sb - top) * coef), jnp.exp2((sc - top) * coef)
            inv = 1.0 / col_sum(eb + ec)
            pb, pc = eb * inv, ec * inv
            dot = col_sum(dpb * pb + dpc * pc)
            dsb = (pb * (dpb - dot) * scale).astype(BF16)
            dsc = (pc * (dpc - dot) * scale).astype(BF16)
            p0 = jnp.concatenate([pa.astype(BF16), pb.astype(BF16)], axis=1)
            second.append((h, cols, p0, pc.astype(BF16), dsa, dsb, dsc))
        for h, cols, p0, p1, dsa, dsb, dsc in second:
            q, k, d = q_ref[:, cols], k_ref[:, cols], d_ref[:, cols]
            emit(nn_dot(p0, d), nn_dot(p1, d[half:]), h + 2 * width)
            emit(nn_dot(jnp.concatenate([dsa, dsb], axis=1), q), nn_dot(dsc, q[half:]), h + width)
            emit(tn_dot(dsa, k[:half]), tn_dot(jnp.concatenate([dsb, dsc], axis=0), k), h)


def attn_bwd(grp, qkv, d_att, group, out_groups, width, seq, row0, total, prev):
    rows = qkv.shape[0]
    heads = width // 128
    off = row0 // seq
    in_specs = [pl.BlockSpec((seq, width), lambda i, c, j=j: (i, 3 * group + j)) for j in range(3)]
    in_specs.append(pl.BlockSpec((seq, width), lambda i, c: (i + off, c[0])))
    args = [grp, qkv, qkv, qkv, d_att]
    aliases = {}
    if prev is not None:
        in_specs.append(pl.BlockSpec(memory_space=pl.ANY))
        args.append(prev)
        aliases = {5: 0}
    nheads = rows // seq * heads
    return pl.pallas_call(
        functools.partial(attn_bwd_body, heads, 128 ** -0.5),
        out_shape=(
            jax.ShapeDtypeStruct((total, 3 * width * out_groups), BF16),
            jax.ShapeDtypeStruct((8, 3 * width), F32),
        ),
        grid_spec=pltpu.PrefetchScalarGridSpec(
            num_scalar_prefetch=1,
            grid=(rows // seq,),
            in_specs=in_specs,
            out_specs=(
                pl.BlockSpec((seq, 3 * width), lambda i, c: (i + off, group)),
                pl.BlockSpec((8, 3 * width), lambda i, c: (0, 0)),
            ),
        ),
        input_output_aliases=aliases,
        cost_estimate=pl.CostEstimate(flops=nheads * seq * seq * 128 * 20, bytes_accessed=14 * rows * width, transcendentals=nheads * seq * seq),
        name="attn_bwd",
    )(*args)


def out_body(col_ref, att_ref, w_ref, x_ref, b_ref, out_ref):
    out_ref[...] = (x_ref[...].astype(F32) + nn_dot(att_ref[...], w_ref[...]) + b_ref[...]).astype(BF16)


def out_rows(col, att, w_o, x_loc, bias):
    tokens, full = att.shape
    width = w_o.shape[1]
    blk, wide = 1024, 1024
    nblk = tokens // blk
    place = pl.BlockSpec((blk, wide), lambda n, m, c: (m + c[0] * nblk, n))
    return pl.pallas_call(
        out_body,
        out_shape=jax.ShapeDtypeStruct((2 * tokens, width), BF16),
        grid_spec=pltpu.PrefetchScalarGridSpec(
            num_scalar_prefetch=1,
            grid=(width // wide, nblk),
            in_specs=[
                pl.BlockSpec((blk, full), lambda n, m, c: (m, 0)),
                pl.BlockSpec((full, wide), lambda n, m, c: (0, n)),
                place,
                pl.BlockSpec((1, wide), lambda n, m, c: (0, n)),
            ],
            out_specs=place,
        ),
        compiler_params=pltpu.CompilerParams(vmem_limit_bytes=56 * 1024 * 1024),
        cost_estimate=pl.CostEstimate(flops=2 * tokens * full * width, bytes_accessed=4 * tokens * full, transcendentals=0),
        name="out_rows",
    )(col, att, w_o, x_loc, bias)


def regroup_body(src_ref, out_ref):
    wide = src_ref.shape[1] // 6
    for j in range(2):
        for t in range(3):
            out_ref[:, (3 * j + t) * wide:(3 * j + t + 1) * wide] = src_ref[:, (2 * t + j) * wide:(2 * t + j + 1) * wide]


def regroup(val):
    rows, width = val.shape
    spec = pl.BlockSpec((256, width), lambda i: (i, 0))
    return pl.pallas_call(
        regroup_body,
        out_shape=jax.ShapeDtypeStruct(val.shape, val.dtype),
        grid=(rows // 256,),
        in_specs=[spec],
        out_specs=spec,
        cost_estimate=pl.CostEstimate(flops=rows * width, bytes_accessed=4 * rows * width, transcendentals=0),
        name="regroup",
    )(val)


def join_body(side, pos_ref, own_ref, recv_ref, half_ref, rest_ref, *rest):
    out_ref = rest[-1]
    wide = own_ref.shape[1] // 3
    mine = pos_ref[0] == side

    def cols(t, j):
        return pl.ds((2 * t + j) * wide, wide)

    for src, flag in ((own_ref, mine), (recv_ref, jnp.logical_not(mine))):
        @pl.when(flag)
        def _(src=src):
            for t in range(3):
                out_ref[:, cols(t, 0)] = src[:, t * wide:(t + 1) * wide]

    for t in range(3):
        part = pl.ds(t * wide, wide)
        out_ref[:, cols(t, 1)] = (half_ref[:, part].astype(F32) + rest_ref[:, part].astype(F32)).astype(BF16)


def join(side, pos, own, recv, half, rest, prev):
    rows, width = own.shape
    blk = 128
    steps = rows // blk
    own_spec = pl.BlockSpec((blk, width), lambda i, p: (jnp.where(p[0] == side, i, 0), 0))
    recv_spec = pl.BlockSpec((blk, width), lambda i, p: (jnp.where(p[0] == side, 0, i), 0))
    full_spec = pl.BlockSpec((blk, width), lambda i, p: (i, 0))
    in_specs = [own_spec, recv_spec, full_spec, full_spec]
    args = [pos, own, recv, half, rest]
    aliases = {}
    if prev is not None:
        in_specs.append(pl.BlockSpec(memory_space=pl.ANY))
        args.append(prev)
        aliases = {5: 0}
    return pl.pallas_call(
        functools.partial(join_body, side),
        out_shape=jax.ShapeDtypeStruct((2 * rows, 2 * width), BF16),
        grid_spec=pltpu.PrefetchScalarGridSpec(
            num_scalar_prefetch=1,
            grid=(steps,),
            in_specs=in_specs,
            out_specs=pl.BlockSpec((blk, 2 * width), lambda i, p: (i + side * steps, 0)),
        ),
        input_output_aliases=aliases,
        cost_estimate=pl.CostEstimate(flops=rows * width, bytes_accessed=10 * rows * width, transcendentals=0),
        name="join",
    )(*args)


def solution(mesh):
    act_spec = P(("depth", "row"), None, "col")
    mat_spec = P("row", "col")
    vec_spec = P("col")
    bias_spec = P("col", None)

    def swap(val, axis):
        return lax.ppermute(val, axis, SWAP)

    def tie(val, *deps):
        return lax.optimization_barrier((val,) + deps)[0]

    def gather(val, axes):
        return lax.all_gather(val, axes, axis=0, tiled=True)

    def scatter(val, axes):
        return lax.psum_scatter(val, axes, scatter_dimension=0, tiled=True)

    def block(x, ln_g, ln_b, w_qkv, b_qkv, w_o, b_o, d_y):
        num_seq, seq, width = x.shape
        half = num_seq // 2 * seq
        tokens = num_seq * seq
        piece = w_qkv.shape[0] // 2
        hw = width // 2
        col = lax.axis_index("col")
        dep = lax.axis_index("depth")
        other = 1 - col

        def grp_s(val):
            return jnp.reshape(val, (1,)).astype(jnp.int32)

        x2 = x.reshape(tokens, width)
        dy2 = d_y.reshape(tokens, width)
        col_arr, oth_arr, dep_arr = grp_s(col), grp_s(other), grp_s(dep)
        own_grp = [grp_s(col * 2 + j) for j in range(2)]
        oth_grp = [grp_s(other * 2 + j) for j in range(2)]

        def group_cols(val, j):
            return [val[:, t * width + j * hw:t * width + (j + 1) * hw] for t in range(3)]

        def slab(j):
            part = lax.dynamic_slice_in_dim(w_qkv, dep * piece, piece, 0)
            return jnp.concatenate(group_cols(part, j), axis=1)

        def send(val, axis="col"):
            return swap(val, axis)

        nb = hw // 128
        bias = jnp.concatenate([b_qkv[(2 * t + j) * nb:(2 * t + j + 1) * nb] for j in range(2) for t in range(3)], axis=0)
        vecs = jnp.concatenate([ln_g.reshape(-1, 128), ln_b.reshape(-1, 128), b_o.reshape(-1, 128), bias], axis=0)
        rows2 = half // 2
        x_out = [lax.dynamic_slice_in_dim(x2, other * half, rows2, 0)]
        vecs = tie(vecs, x_out[0])
        vecs_r = send(vecs)
        slab_a = tie(slab(0), x_out[0])
        x_out.append(lax.dynamic_slice_in_dim(tie(x2, slab_a), other * half + rows2, rows2, 0))
        slab_b = tie(slab(1), x_out[1])
        wo_out = lax.dynamic_slice_in_dim(tie(w_o, slab_b), dep * piece, piece, 0)
        dy_out = lax.dynamic_slice_in_dim(tie(dy2, wo_out), other * half, half, 0)
        x_recv = [send(x_out[0])]
        wa_in = send(slab_a)
        x_recv.append(send(x_out[1]))
        wb_in = send(slab_b)
        wo_in = send(wo_out)
        dy_recv = send(dy_out)
        w_perm = regroup(tie(w_qkv, dy_out))
        wo_own = gather(w_o, "row")
        w_own = gather(w_perm, "row")

        nv = width // 128
        first = col == 0

        db_o = jnp.sum(dy2.astype(F32), axis=0)
        wq_oth = [None, None]
        qkv_oth = [None, None]
        dqkv_oth = [None, None]
        sum_oth = [None, None]

        def held(*vals):
            return lax.optimization_barrier(vals)

        def project(j):
            return (nn_dot(xn, wq_oth[j]) + bq_oth[j]).astype(BF16)

        def weight_grad(lhs, rhs):
            return tn_dot(lhs, rhs).astype(BF16)

        dy_own = lax.dynamic_slice_in_dim(tie(dy2, dy_out), col * half, half, 0)
        datt_part = nt_dot(tie(dy_own, w_perm), wo_own)

        vecs_r = tie(vecs_r, datt_part)

        def both(lo, hi):
            a = vecs[lo:hi].reshape(1, -1)
            b = vecs_r[lo:hi].reshape(1, -1)
            return jnp.concatenate([jnp.where(first, a, b), jnp.where(first, b, a)], axis=1)

        g_full = both(0, nv)
        b_full = both(nv, 2 * nv)
        bo_oth = vecs_r[2 * nv:3 * nv].reshape(-1)
        bq_own = bias.reshape(-1)
        bq_oth = vecs_r[3 * nv:].reshape(2, 3 * hw)

        xn, stats = ln_fwd(col_arr, tie(x2, datt_part, db_o), x_recv[0], g_full, b_full, 0, half, None)
        qkv_own = [(nn_dot(xn[:rows2], w_own) + bq_own).astype(BF16)]
        wa_in, xn, qkv_own[0] = held(wa_in, xn, qkv_own[0])
        wq_oth[0] = gather(wa_in, ("row", "depth"))
        xn, stats = ln_fwd(col_arr, x2, x_recv[1], g_full, b_full, rows2, half, (xn, stats))
        qkv_own.append((nn_dot(xn[rows2:], w_own) + bq_own).astype(BF16))
        att = None
        for i in range(2):
            att = attn_fwd(own_grp[0], qkv_own[i] if i else tie(qkv_own[0], qkv_own[1]), 2, hw, seq, i * rows2, half, att)
        wb_in, xn, att = held(wb_in, xn, att)
        wq_oth[1] = gather(wb_in, ("row", "depth"))
        qkv_oth[0] = project(0)
        att = attn_fwd(oth_grp[0], qkv_oth[0], 1, hw, seq, 0, half, att)
        wo_in, att, xn = held(wo_in, att, xn)
        wo_oth = gather(wo_in, ("row", "depth"))
        qkv_oth[1] = project(1)
        att = attn_fwd(oth_grp[1], qkv_oth[1], 1, hw, seq, 0, half, att)
        x_all = jnp.concatenate(x_recv, axis=0)
        y_send = (x_all.astype(F32) + nn_dot(att, wo_oth) + bo_oth).astype(BF16)
        y_recv = send(y_send)
        y = out_rows(col_arr, tie(att, y_send), wo_own, x2, b_o.reshape(1, -1))

        def back_far(j, gate):
            dqkv_oth[j], sum_oth[j] = attn_bwd(oth_grp[j], tie(qkv_oth[j], gate), d_att, 0, 1, hw, seq, 0, half, None)

        def back_own(j, gate, prev):
            total = 0.0
            for i in range(2):
                prev, part = attn_bwd(own_grp[j], tie(qkv_own[i], gate), d_att, j, 2, hw, seq, i * rows2, half, prev)
                total = total + part
            return prev, total

        wide = 3 * hw
        sum_own = [None, None]
        d_att = (nt_dot(tie(dy_recv, y), wo_oth) + datt_part).astype(BF16)
        dwo_far = weight_grad(tie(att, d_att), dy_recv)
        red_of = scatter(dwo_far, "row")
        back_far(0, dwo_far)
        dw_a = weight_grad(xn, dqkv_oth[0])
        red_a = scatter(dw_a, ("row", "depth"))
        red_of, dw_a = held(red_of, dw_a)
        far_o = send(red_of)
        dwo_near = weight_grad(tie(att, dw_a), dy_own)
        red_on = scatter(dwo_near, "row")
        back_far(1, dwo_near)
        dw_b = weight_grad(xn, dqkv_oth[1])
        red_b = scatter(dw_b, "row")
        far_o, red_on, red_a, dw_b = held(far_o, red_on, red_a, dw_b)
        far_a = send(red_a)
        half_o = (red_on.astype(F32) + far_o.astype(F32)).astype(BF16)
        half_r = send(half_o, "depth")
        dqkv_own, sum_own[0] = back_own(0, half_o, None)
        dw_oa = weight_grad(xn, dqkv_own[:, :wide])
        red_oa = scatter(dw_oa, ("row", "depth"))
        red_b, dw_oa = held(red_b, dw_oa)
        far_b = send(red_b)
        dqkv_own, sum_own[1] = back_own(1, dw_oa, dqkv_own)
        dw_ob = weight_grad(xn, dqkv_own[:, wide:])
        red_ob = scatter(dw_ob, "row")

        unit = half // 6
        parts = (unit, unit, 2 * unit, unit, unit)
        dx, gate, lo = None, dw_ob, 0
        dx_recv, sums_n = [], []
        grads = [dqkv_own, *dqkv_oth]
        for part, rows in enumerate(parts):
            grads[1] = tie(grads[1], gate)
            dx, dx_send, dg8, db8 = dx_part(col_arr, grads, (w_own, *wq_oth), x2, x_recv, dy2, dy_recv, stats, g_full, lo, rows, dx)
            lo += rows
            sums_n.append((dg8, db8))
            dx_recv.append(send(dx_send))
            gate = dx_send
            if part == 0:
                far_a, red_oa, gate = held(far_a, red_oa, gate)
                half_a = (red_oa.astype(F32) + far_a.astype(F32)).astype(BF16)
                rest_a = send(half_a, "depth")
                gate = half_a
            if part == 1:
                far_b, red_ob, gate = held(far_b, red_ob, gate)
                half_b, rest_b = [], []
                for i in range(2):
                    part_rows = slice(i * piece, (i + 1) * piece)
                    half_b.append((tie(red_ob, gate)[part_rows].astype(F32) + far_b[part_rows].astype(F32)).astype(BF16))
                    rest_b.append(send(half_b[i], "depth"))
                    gate = half_b[i]

        def natural(pair):
            vals = [jnp.sum(s, axis=0).reshape(3, hw) for s in pair]
            return jnp.concatenate([vals[j][t] for t in range(3) for j in range(2)])

        dg = jnp.sum(sum(pair[0] for pair in sums_n), axis=0)
        dbn = jnp.sum(sum(pair[1] for pair in sums_n), axis=0)
        far = jnp.concatenate([natural(sum_oth), lax.dynamic_slice_in_dim(dg, other * width, width), lax.dynamic_slice_in_dim(dbn, other * width, width)])
        near = jnp.concatenate([natural(sum_own), lax.dynamic_slice_in_dim(dg, col * width, width), lax.dynamic_slice_in_dim(dbn, col * width, width)])
        near = near.reshape(-1, 128)
        far = send(far.reshape(-1, 128))
        y = lax.dynamic_update_slice(y, tie(y_recv, gate), (other * half, 0))
        far, y = held(far, y)
        total = jnp.concatenate([near + far, db_o.reshape(-1, 128)], axis=0)
        row_in = send(total, "row")
        dw_o = (tie(half_o, y, total).astype(F32) + half_r.astype(F32)).astype(BF16)
        row_in, dw_o = held(row_in, dw_o)
        total = total + row_in
        dep_in = send(total, "depth")
        place, lo = dw_o, 0
        for part, rows in enumerate(parts):
            if part == 3:
                dw_qkv = join(0, dep_arr, half_a, tie(rest_a, dx), half_b[0], rest_b[0], None)
                dw_qkv = join(1, dep_arr, half_a, rest_a, half_b[1], rest_b[1], dw_qkv)
                place = dw_qkv
            dx = lax.dynamic_update_slice(dx, tie(dx_recv[part], place), (other * half + lo, 0))
            lo += rows
        total = total + tie(dep_in, dx)
        db_o = total[-nv:]
        nq = 3 * nv
        return (
            y.reshape(x.shape),
            dx.reshape(x.shape),
            dw_qkv,
            total[:nq],
            dw_o,
            db_o.reshape(-1),
            total[nq:nq + nv].reshape(-1),
            total[nq + nv:nq + 2 * nv].reshape(-1),
        )

    return jax.shard_map(
        block,
        mesh=mesh,
        in_specs=(act_spec, vec_spec, vec_spec, mat_spec, bias_spec, mat_spec, vec_spec, act_spec),
        out_specs=(act_spec, act_spec, mat_spec, bias_spec, mat_spec, vec_spec, vec_spec, vec_spec),
        check_vma=False,
    )
```

```python
import functools

import jax
import jax.numpy as jnp
from jax import lax
from jax.experimental import pallas as pl
from jax.experimental.pallas import tpu as pltpu
from jax.sharding import PartitionSpec as P


LN_EPS = 1e-5
SWAP = [(0, 1), (1, 0)]
F32 = jnp.float32
BF16 = jnp.bfloat16
LOG2E = 1.4426950408889634


def nt_dot(lhs, rhs):
    return lax.dot_general(lhs, rhs, (((1,), (1,)), ((), ())), preferred_element_type=F32)


def tn_dot(lhs, rhs):
    return lax.dot_general(lhs, rhs, (((0,), (0,)), ((), ())), preferred_element_type=F32)


def nn_dot(lhs, rhs):
    return lax.dot_general(lhs, rhs, (((1,), (0,)), ((), ())), preferred_element_type=F32)


def row_sum(val):
    return jnp.sum(val, -1, keepdims=True)


def group_rows(i, unroll, step):
    return [pl.ds(pl.multiple_of((i * unroll + u) * step, step), step) for u in range(unroll)]


def ln_fwd_body(col_ref, own_ref, recv_ref, g_ref, b_ref, *rest):
    xn_ref, stat_ref = rest[-2:]
    width = own_ref.shape[1]
    inv_n = 1.0 / (2 * width)
    col = col_ref[0]
    own_cols = pl.ds(pl.multiple_of(col * width, width), width)
    far_cols = pl.ds(pl.multiple_of((1 - col) * width, width), width)
    step, unroll = 16, 4

    @pl.loop(0, own_ref.shape[0] // (step * unroll))
    def _(i):
        groups = group_rows(i, unroll, step)
        means = [row_sum(own_ref[r, :].astype(F32) + recv_ref[r, :].astype(F32)) * inv_n for r in groups]
        invs = []
        for r, mean in zip(groups, means):
            own = own_ref[r, :].astype(F32) - mean
            far = recv_ref[r, :].astype(F32) - mean
            invs.append(lax.rsqrt(row_sum(own * own + far * far) * inv_n + LN_EPS))
        for r, mean, inv in zip(groups, means, invs):
            stat_ref[r, :128] = jnp.broadcast_to(mean, (step, 128))
            stat_ref[r, 128:] = jnp.broadcast_to(inv, (step, 128))
            for src, cols in ((own_ref, own_cols), (recv_ref, far_cols)):
                hat = (src[r, :].astype(F32) - mean) * inv
                xn_ref[r, cols] = (hat * g_ref[:, cols] + b_ref[:, cols]).astype(BF16)


def ln_fwd(col, x_loc, x_recv, g_full, b_full, row0, total, prev):
    rows, width = x_recv.shape
    blk = 256
    nall = total // blk
    off = row0 // blk
    in_specs = [
        pl.BlockSpec((blk, width), lambda i, c: (i + off + c[0] * nall, 0)),
        pl.BlockSpec((blk, width), lambda i, c: (i, 0)),
        pl.BlockSpec((1, 2 * width), lambda i, c: (0, 0)),
        pl.BlockSpec((1, 2 * width), lambda i, c: (0, 0)),
    ]
    args = [col, x_loc, x_recv, g_full, b_full]
    aliases = {}
    if prev is not None:
        in_specs.extend([pl.BlockSpec(memory_space=pl.ANY)] * 2)
        args.extend(prev)
        aliases = {5: 0, 6: 1}
    return pl.pallas_call(
        ln_fwd_body,
        out_shape=(jax.ShapeDtypeStruct((total, 2 * width), BF16), jax.ShapeDtypeStruct((total, 256), F32)),
        grid_spec=pltpu.PrefetchScalarGridSpec(
            num_scalar_prefetch=1,
            grid=(rows // blk,),
            in_specs=in_specs,
            out_specs=(pl.BlockSpec((blk, 2 * width), lambda i, c: (i + off, 0)), pl.BlockSpec((blk, 256), lambda i, c: (i + off, 0))),
        ),
        input_output_aliases=aliases,
        cost_estimate=pl.CostEstimate(flops=20 * rows * 2 * width, bytes_accessed=8 * rows * width, transcendentals=0),
        name="ln_fwd",
    )(*args)


def ln_bwd_rows(dxn_ref, sides, stat_ref, g_ref, dg_ref, db_ref):
    rows = dxn_ref.shape[0]
    inv_n = 1.0 / dxn_ref.shape[1]
    step, unroll = 16, 4

    def fold(val):
        return jnp.sum(val.reshape(val.shape[0] // 8, 8, val.shape[1]), axis=0)

    @pl.loop(0, rows // (step * unroll))
    def _(i):
        groups = group_rows(i, unroll, step)
        full = []
        for r in groups:
            mean, inv = stat_ref[r, 0:1], stat_ref[r, 128:129]
            m1, m2 = 0.0, 0.0
            for x_ref, _, _, cols in sides:
                part = dxn_ref[r, cols] * g_ref[:, cols]
                m1 = m1 + part
                m2 = m2 + part * (x_ref[r, :].astype(F32) - mean)
            full.append((mean, inv, row_sum(m1) * inv_n, row_sum(m2) * inv_n * inv))
        for x_ref, dy_ref, dx_ref, cols in sides:
            sum_g = sum_b = None
            for r, (mean, inv, m1, m2) in zip(groups, full):
                hat = (x_ref[r, :].astype(F32) - mean) * inv
                d = dxn_ref[r, cols]
                add_g, add_b = fold(d * hat), fold(d)
                sum_g = add_g if sum_g is None else sum_g + add_g
                sum_b = add_b if sum_b is None else sum_b + add_b
                dx_ref[r, :] = (dy_ref[r, :].astype(F32) + inv * (d * g_ref[:, cols] - m1 - hat * m2)).astype(BF16)
            dg_ref[:, cols] += sum_g
            db_ref[:, cols] += sum_b


def dx_body(row0, half, steps, with_y, col_ref, d_own, d_a, d_b, w_own, w_a, w_b, x_ref, x0_ref, x1_ref, dy_ref, dyr_ref, stat_ref, g_ref, *rest):
    if with_y:
        yr0_ref, yr1_ref, y_ref, y_buf, y_sems = rest[-16], rest[-15], rest[-9], rest[-2], rest[-1]
        rest = rest[:-9] + rest[-8:-2]
    dx_ref, send_ref, dg_ref, db_ref, acc, w_buf, d_buf, ln_buf, sems, ln_sems = rest[-10:]
    m = pl.program_id(0)
    blk, wide = d_buf.shape[1:]
    width = x_ref.shape[1]
    col = col_ref[0]
    sources, count = [], 0
    for d, w in ((d_own, w_own), (d_a, w_a), (d_b, w_b)):
        chunks = d.shape[1] // wide
        sources.append((d, w, count, chunks))
        count += chunks

    def copies(d, w, block, chunk, slot):
        rows = pl.ds(pl.multiple_of(row0 + block * blk, blk), blk)
        cols = pl.ds(pl.multiple_of(chunk * wide, wide), wide)
        return (
            pltpu.make_async_copy(w.at[:, cols], w_buf.at[slot], sems.at[0, slot]),
            pltpu.make_async_copy(d.at[rows, cols], d_buf.at[slot], sems.at[1, slot]),
        )

    def fetch(block, chunk, slot):
        for d, w, lo, chunks in sources:
            @pl.when((chunk >= lo) & (chunk < lo + chunks))
            def _():
                for copy in copies(d, w, block, chunk - lo, slot):
                    copy.start()

    @pl.when(m == 0)
    def _():
        dg_ref[...] = jnp.zeros_like(dg_ref)
        db_ref[...] = jnp.zeros_like(db_ref)
        fetch(0, 0, 0)

    row = row0 + m * blk
    own_rows = pl.ds(pl.multiple_of(col * half + row, blk), blk)
    far_rows = pl.ds(pl.multiple_of(row, blk), blk)
    pair = half // 2
    x0_rows = pl.ds(pl.multiple_of(jnp.minimum(row, pair - blk), blk), blk)
    x1_rows = pl.ds(pl.multiple_of(jnp.maximum(row - pair, 0), blk), blk)

    def ln_copy(i, src):
        return pltpu.make_async_copy(src, ln_buf.at[i], ln_sems.at[i])

    ln_copy(0, x_ref.at[own_rows]).start()
    ln_copy(2, dy_ref.at[own_rows]).start()
    ln_copy(3, dyr_ref.at[far_rows]).start()

    @pl.when(row < pair)
    def _():
        ln_copy(1, x0_ref.at[x0_rows]).start()

    @pl.when(row >= pair)
    def _():
        ln_copy(1, x1_ref.at[x1_rows]).start()

    acc[...] = jnp.zeros_like(acc)

    y_blocks = steps * count // 2
    y_rows = half // (2 * y_blocks)

    def y_in(t, src, block):
        place = pl.ds(pl.multiple_of(block * y_rows, y_rows), y_rows)
        return pltpu.make_async_copy(src.at[place], y_buf.at[lax.rem(t, 2)], y_sems.at[0, lax.rem(t, 2)])

    def y_out(t):
        place = pl.ds(pl.multiple_of((1 - col) * half + t * y_rows, y_rows), y_rows)
        return pltpu.make_async_copy(y_buf.at[lax.rem(t, 2)], y_ref.at[place], y_sems.at[1, lax.rem(t, 2)])

    @pl.loop(0, count)
    def _(k):
        t = m * count + k
        slot = lax.rem(t, 2)
        if with_y:
            @pl.when(t >= 2)
            def _():
                y_out(t - 2).wait()

            @pl.when(t < y_blocks)
            def _():
                y_in(t, yr0_ref, jnp.minimum(t, y_blocks - 1)).start()

            @pl.when(t >= y_blocks)
            def _():
                y_in(t, yr1_ref, jnp.maximum(t - y_blocks, 0)).start()

            @pl.when(t >= 1)
            def _():
                y_in(t - 1, yr0_ref, 0).wait()
                y_out(t - 1).start()

        @pl.when(k + 1 < count)
        def _():
            fetch(m, k + 1, 1 - slot)

        @pl.when((k + 1 == count) & (m + 1 < steps))
        def _():
            fetch(m + 1, 0, 1 - slot)

        for copy in copies(d_a, w_a, 0, 0, slot):
            copy.wait()
        acc[...] += nt_dot(d_buf[slot], w_buf[slot])

    for i in range(4):
        ln_copy(i, dyr_ref.at[far_rows]).wait()
    if with_y:
        @pl.when(m == steps - 1)
        def _():
            last = steps * count - 1
            y_in(last, yr0_ref, 0).wait()
            y_out(last).start()
            y_out(last - 1).wait()
            y_out(last).wait()

    own_cols = pl.ds(pl.multiple_of(col * width, width), width)
    far_cols = pl.ds(pl.multiple_of((1 - col) * width, width), width)
    sides = ((ln_buf.at[0], ln_buf.at[2], dx_ref, own_cols), (ln_buf.at[1], ln_buf.at[3], send_ref, far_cols))
    ln_bwd_rows(acc, sides, stat_ref, g_ref, dg_ref, db_ref)


def dx_part(col, dqkv, weights, x_loc, x_recv, dy_loc, dy_recv, stats, g_full, row0, rows, dx_prev, y_pair=None):
    total, width = dy_recv.shape
    blk, wide = 384, 1024
    off = row0 // blk
    nall = total // blk
    own_spec = pl.BlockSpec((blk, width), lambda i, c: (i + off + c[0] * nall, 0))
    sums_spec = pl.BlockSpec((8, 2 * width), lambda i, c: (0, 0))
    any_spec = pl.BlockSpec(memory_space=pl.ANY)
    in_specs = [any_spec] * 11 + [pl.BlockSpec((blk, 256), lambda i, c: (i + off, 0)), pl.BlockSpec((1, 2 * width), lambda i, c: (0, 0))]
    args = [col, *dqkv, *weights, x_loc, *x_recv, dy_loc, dy_recv, stats, g_full]
    aliases = {}
    if dx_prev is not None:
        in_specs.append(any_spec)
        args.append(dx_prev)
        aliases = {14: 0}
    out_shape = [
        jax.ShapeDtypeStruct((2 * total, width), BF16),
        jax.ShapeDtypeStruct((rows, width), BF16),
        jax.ShapeDtypeStruct((8, 2 * width), F32),
        jax.ShapeDtypeStruct((8, 2 * width), F32),
    ]
    out_specs = [own_spec, pl.BlockSpec((blk, width), lambda i, c: (i, 0)), sums_spec, sums_spec]
    scratch = [
        pltpu.VMEM((blk, 2 * width), F32),
        pltpu.VMEM((2, 2 * width, wide), BF16),
        pltpu.VMEM((2, blk, wide), BF16),
        pltpu.VMEM((4, blk, width), BF16),
        pltpu.SemaphoreType.DMA((2, 2)),
        pltpu.SemaphoreType.DMA((4,)),
    ]
    depth = sum(d.shape[1] for d in dqkv)
    if y_pair is not None:
        in_specs.extend([any_spec] * 3)
        args.extend(y_pair)
        aliases[len(args) - 1] = 4
        out_shape.append(jax.ShapeDtypeStruct(y_pair[2].shape, BF16))
        out_specs.append(any_spec)
        scratch.extend([pltpu.VMEM((2, total * blk * wide // (rows * depth), width), BF16), pltpu.SemaphoreType.DMA((2, 2))])
    return pl.pallas_call(
        functools.partial(dx_body, row0, total, rows // blk, y_pair is not None),
        out_shape=out_shape,
        grid_spec=pltpu.PrefetchScalarGridSpec(num_scalar_prefetch=1, grid=(rows // blk,), in_specs=in_specs, out_specs=out_specs, scratch_shapes=scratch),
        input_output_aliases=aliases,
        compiler_params=pltpu.CompilerParams(vmem_limit_bytes=60 * 1024 * 1024),
        cost_estimate=pl.CostEstimate(flops=4 * rows * width * depth, bytes_accessed=(rows // blk) * 4 * width * depth, transcendentals=0),
        name="dx_part",
    )(*args)


def attn_fwd_body(heads, scale, grp_ref, q_ref, k_ref, v_ref, *rest):
    out_ref = rest[-1]
    half = q_ref.shape[0] // 2
    causal = lax.broadcasted_iota(jnp.int32, (half, half), 0) >= lax.broadcasted_iota(jnp.int32, (half, half), 1)
    unroll = 8
    coef = scale * LOG2E

    @pl.loop(0, heads // unroll)
    def _(i):
        scores = []
        for j in range(unroll):
            cols = pl.ds(pl.multiple_of((i * unroll + j) * 128, 128), 128)
            k = k_ref[:, cols]
            scores.append((cols, nt_dot(q_ref[:half, cols], k[:half]), nt_dot(q_ref[half:, cols], k)))
        probs = []
        for cols, s0, s1 in scores:
            sa = jnp.where(causal, s0, -1e30)
            ea = jnp.exp2((sa - jnp.max(sa, -1, keepdims=True)) * coef)
            pa = (ea * (1.0 / row_sum(ea))).astype(BF16)
            sb, sc = s1[:, :half], jnp.where(causal, s1[:, half:], -1e30)
            top = jnp.max(jnp.maximum(sb, sc), -1, keepdims=True)
            eb, ec = jnp.exp2((sb - top) * coef), jnp.exp2((sc - top) * coef)
            inv = 1.0 / row_sum(eb + ec)
            probs.append((cols, pa, jnp.concatenate([(eb * inv).astype(BF16), (ec * inv).astype(BF16)], axis=1)))
        for cols, p0, p1 in probs:
            v = v_ref[:, cols]
            out_ref[:half, cols] = nn_dot(p0, v[:half]).astype(BF16)
            out_ref[half:, cols] = nn_dot(p1, v).astype(BF16)


def attn_fwd(grp, qkv, groups, width, seq, row0, rows, prev):
    heads = width // 128
    off = row0 // seq
    in_specs = [pl.BlockSpec((seq, width), lambda g, i, c, j=j: (i + off, 3 * g + j)) for j in range(3)]
    args = [grp, qkv, qkv, qkv]
    aliases = {}
    if prev is not None:
        in_specs.append(pl.BlockSpec(memory_space=pl.ANY))
        args.append(prev)
        aliases = {4: 0}
    nheads = rows // seq * heads * groups
    return pl.pallas_call(
        functools.partial(attn_fwd_body, heads, 128 ** -0.5),
        out_shape=jax.ShapeDtypeStruct((qkv.shape[0], 4096), BF16),
        grid_spec=pltpu.PrefetchScalarGridSpec(
            num_scalar_prefetch=1,
            grid=(groups, rows // seq),
            in_specs=in_specs,
            out_specs=pl.BlockSpec((seq, width), lambda g, i, c: (i + off, c[0] + g)),
        ),
        input_output_aliases=aliases,
        cost_estimate=pl.CostEstimate(flops=nheads * seq * seq * 128 * 8, bytes_accessed=8 * rows * width * groups, transcendentals=nheads * seq * seq),
        name="attn_fwd",
    )(*args)


def attn_bwd_body(heads, scale, grp_ref, q_ref, k_ref, v_ref, d_ref, *rest):
    dq_ref, sum_ref = rest[-2:]
    seq, width = q_ref.shape
    half = seq // 2
    causal = lax.broadcasted_iota(jnp.int32, (half, half), 1) >= lax.broadcasted_iota(jnp.int32, (half, half), 0)
    unroll = 8
    coef = scale * LOG2E

    @pl.when(pl.program_id(0) == 0)
    def _():
        sum_ref[...] = jnp.zeros_like(sum_ref)

    def col_sum(val):
        return jnp.sum(val, 0, keepdims=True)

    def emit(top, bottom, start):
        cols = pl.ds(pl.multiple_of(start, 128), 128)
        dq_ref[:half, cols] = top.astype(BF16)
        dq_ref[half:, cols] = bottom.astype(BF16)
        sum_ref[:, cols] += jnp.sum((top + bottom).reshape(half // 8, 8, 128), axis=0)

    @pl.loop(0, heads // unroll)
    def _(i):
        first = []
        for j in range(unroll):
            h = (i * unroll + j) * 128
            cols = pl.ds(pl.multiple_of(h, 128), 128)
            q, k, v, d = q_ref[:, cols], k_ref[:, cols], v_ref[:, cols], d_ref[:, cols]
            first.append((h, cols, nt_dot(k[:half], q), nt_dot(k[half:], q[half:]), nt_dot(v[:half], d), nt_dot(v[half:], d[half:])))
        second = []
        for h, cols, s0, s1, dp0, dpc in first:
            sa = jnp.where(causal, s0[:, :half], -1e30)
            ea = jnp.exp2((sa - jnp.max(sa, 0, keepdims=True)) * coef)
            pa = ea * (1.0 / col_sum(ea))
            dpa, dpb = dp0[:, :half], dp0[:, half:]
            dsa = (pa * (dpa - col_sum(dpa * pa)) * scale).astype(BF16)
            sb, sc = s0[:, half:], jnp.where(causal, s1, -1e30)
            top = jnp.max(jnp.maximum(sb, sc), 0, keepdims=True)
            eb, ec = jnp.exp2((sb - top) * coef), jnp.exp2((sc - top) * coef)
            inv = 1.0 / col_sum(eb + ec)
            pb, pc = eb * inv, ec * inv
            dot = col_sum(dpb * pb + dpc * pc)
            dsb = (pb * (dpb - dot) * scale).astype(BF16)
            dsc = (pc * (dpc - dot) * scale).astype(BF16)
            p0 = jnp.concatenate([pa.astype(BF16), pb.astype(BF16)], axis=1)
            second.append((h, cols, p0, pc.astype(BF16), dsa, dsb, dsc))
        for h, cols, p0, p1, dsa, dsb, dsc in second:
            q, k, d = q_ref[:, cols], k_ref[:, cols], d_ref[:, cols]
            emit(nn_dot(p0, d), nn_dot(p1, d[half:]), h + 2 * width)
            emit(nn_dot(jnp.concatenate([dsa, dsb], axis=1), q), nn_dot(dsc, q[half:]), h + width)
            emit(tn_dot(dsa, k[:half]), tn_dot(jnp.concatenate([dsb, dsc], axis=0), k), h)


def attn_bwd(grp, qkv, d_att, group, out_groups, width, seq, row0, total, prev):
    rows = qkv.shape[0]
    heads = width // 128
    off = row0 // seq
    in_specs = [pl.BlockSpec((seq, width), lambda i, c, j=j: (i, 3 * group + j)) for j in range(3)]
    in_specs.append(pl.BlockSpec((seq, width), lambda i, c: (i + off, c[0])))
    args = [grp, qkv, qkv, qkv, d_att]
    aliases = {}
    if prev is not None:
        in_specs.append(pl.BlockSpec(memory_space=pl.ANY))
        args.append(prev)
        aliases = {5: 0}
    nheads = rows // seq * heads
    return pl.pallas_call(
        functools.partial(attn_bwd_body, heads, 128 ** -0.5),
        out_shape=(
            jax.ShapeDtypeStruct((total, 3 * width * out_groups), BF16),
            jax.ShapeDtypeStruct((8, 3 * width), F32),
        ),
        grid_spec=pltpu.PrefetchScalarGridSpec(
            num_scalar_prefetch=1,
            grid=(rows // seq,),
            in_specs=in_specs,
            out_specs=(
                pl.BlockSpec((seq, 3 * width), lambda i, c: (i + off, group)),
                pl.BlockSpec((8, 3 * width), lambda i, c: (0, 0)),
            ),
        ),
        input_output_aliases=aliases,
        cost_estimate=pl.CostEstimate(flops=nheads * seq * seq * 128 * 20, bytes_accessed=14 * rows * width, transcendentals=nheads * seq * seq),
        name="attn_bwd",
    )(*args)


def out_early_body(col_ref, a0_ref, a1_ref, a2_ref, w0_ref, w1_ref, w2_ref, out_ref):
    part = nn_dot(a0_ref[...], w0_ref[...]) + nn_dot(a1_ref[...], w1_ref[...])
    out_ref[...] = part + nn_dot(a2_ref[...], w2_ref[...])


def out_early(col, att, w_o):
    tokens = att.shape[0]
    full, width = w_o.shape
    blk = 1024

    def group(k, c):
        return 2 * c[0] + k if k < 2 else 2 * (1 - c[0])

    return pl.pallas_call(
        out_early_body,
        out_shape=jax.ShapeDtypeStruct((tokens, width), F32),
        grid_spec=pltpu.PrefetchScalarGridSpec(
            num_scalar_prefetch=1,
            grid=(width // blk, tokens // blk),
            in_specs=[
                *[pl.BlockSpec((blk, blk), lambda n, m, c, k=k: (m, group(k, c))) for k in range(3)],
                *[pl.BlockSpec((blk, blk), lambda n, m, c, k=k: (group(k, c), n)) for k in range(3)],
            ],
            out_specs=pl.BlockSpec((blk, blk), lambda n, m, c: (m, n)),
        ),
        compiler_params=pltpu.CompilerParams(vmem_limit_bytes=56 * 1024 * 1024),
        cost_estimate=pl.CostEstimate(flops=6 * tokens * blk * width, bytes_accessed=6 * tokens * full, transcendentals=0),
        name="out_early",
    )(col, att, att, att, w_o, w_o, w_o)


def out_body(col_ref, part_ref, att_ref, w_ref, x_ref, b_ref, out_ref):
    out_ref[...] = (x_ref[...].astype(F32) + (part_ref[...] + nn_dot(att_ref[...], w_ref[...])) + b_ref[...]).astype(BF16)


def out_rows(col, part, att, w_o, x_loc, bias):
    tokens, width = part.shape
    blk = 1024
    nblk = tokens // blk
    place = pl.BlockSpec((blk, blk), lambda n, m, c: (m + c[0] * nblk, n))
    return pl.pallas_call(
        out_body,
        out_shape=jax.ShapeDtypeStruct((2 * tokens, width), BF16),
        grid_spec=pltpu.PrefetchScalarGridSpec(
            num_scalar_prefetch=1,
            grid=(width // blk, nblk),
            in_specs=[
                pl.BlockSpec((blk, blk), lambda n, m, c: (m, n)),
                pl.BlockSpec((blk, blk), lambda n, m, c: (m, 2 * (1 - c[0]) + 1)),
                pl.BlockSpec((blk, blk), lambda n, m, c: (2 * (1 - c[0]) + 1, n)),
                place,
                pl.BlockSpec((1, blk), lambda n, m, c: (0, n)),
            ],
            out_specs=place,
        ),
        compiler_params=pltpu.CompilerParams(vmem_limit_bytes=56 * 1024 * 1024),
        cost_estimate=pl.CostEstimate(flops=2 * tokens * blk * width, bytes_accessed=12 * tokens * width, transcendentals=0),
        name="out_rows",
    )(col, part, att, w_o, x_loc, bias)


def weight_grad_body(lhs_ref, rhs_ref, out_ref):
    out_ref[...] = tn_dot(lhs_ref[...], rhs_ref[...]).astype(BF16)


def weight_grad_call(lhs, rhs, col0, cols):
    tokens, full = lhs.shape
    blk = 1024
    off = col0 // blk
    return pl.pallas_call(
        weight_grad_body,
        out_shape=jax.ShapeDtypeStruct((full, cols), BF16),
        grid=(cols // blk, full // blk),
        in_specs=[pl.BlockSpec((tokens, blk), lambda n, m: (0, m)), pl.BlockSpec((tokens, blk), lambda n, m: (0, n + off))],
        out_specs=pl.BlockSpec((blk, blk), lambda n, m: (m, n)),
        compiler_params=pltpu.CompilerParams(vmem_limit_bytes=56 * 1024 * 1024),
        cost_estimate=pl.CostEstimate(flops=2 * tokens * full * cols, bytes_accessed=4 * tokens * full, transcendentals=0),
        name="weight_grad",
    )(lhs, rhs)


def project_body(xn_ref, w_ref, b_ref, *rest):
    rest[-1][...] = (nn_dot(xn_ref[...], w_ref[...]) + b_ref[...]).astype(BF16)


def project_rows(xn, w, bias, row0, rows, prev):
    total, full = xn.shape
    width = w.shape[1]
    blk, wide = 768, 1024
    off = row0 // blk
    in_specs = [
        pl.BlockSpec((blk, full), lambda n, m: (m + off, 0)),
        pl.BlockSpec((full, wide), lambda n, m: (0, n)),
        pl.BlockSpec((1, wide), lambda n, m: (0, n)),
    ]
    args = [xn, w, bias.reshape(1, -1)]
    aliases = {}
    if prev is not None:
        in_specs.append(pl.BlockSpec(memory_space=pl.ANY))
        args.append(prev)
        aliases = {3: 0}
    return pl.pallas_call(
        project_body,
        out_shape=jax.ShapeDtypeStruct((total, width), BF16),
        grid=(width // wide, rows // blk),
        in_specs=in_specs,
        out_specs=pl.BlockSpec((blk, wide), lambda n, m: (m + off, n)),
        input_output_aliases=aliases,
        compiler_params=pltpu.CompilerParams(vmem_limit_bytes=56 * 1024 * 1024),
        cost_estimate=pl.CostEstimate(flops=2 * rows * full * width, bytes_accessed=2 * full * width, transcendentals=0),
        name="project",
    )(*args)


def regroup_body(src_ref, out_ref):
    wide = src_ref.shape[1] // 6
    for j in range(2):
        for t in range(3):
            out_ref[:, (3 * j + t) * wide:(3 * j + t + 1) * wide] = src_ref[:, (2 * t + j) * wide:(2 * t + j + 1) * wide]


def regroup(val):
    rows, width = val.shape
    spec = pl.BlockSpec((256, width), lambda i: (i, 0))
    return pl.pallas_call(
        regroup_body,
        out_shape=jax.ShapeDtypeStruct(val.shape, val.dtype),
        grid=(rows // 256,),
        in_specs=[spec],
        out_specs=spec,
        cost_estimate=pl.CostEstimate(flops=rows * width, bytes_accessed=4 * rows * width, transcendentals=0),
        name="regroup",
    )(val)


def join_body(side, pos_ref, own_ref, recv_ref, half_ref, rest_ref, *rest):
    out_ref = rest[-1]
    wide = own_ref.shape[1] // 3
    mine = pos_ref[0] == side

    def cols(t, j):
        return pl.ds((2 * t + j) * wide, wide)

    for src, flag in ((own_ref, mine), (recv_ref, jnp.logical_not(mine))):
        @pl.when(flag)
        def _(src=src):
            for t in range(3):
                out_ref[:, cols(t, 0)] = src[:, t * wide:(t + 1) * wide]

    for t in range(3):
        part = pl.ds(t * wide, wide)
        out_ref[:, cols(t, 1)] = (half_ref[:, part].astype(F32) + rest_ref[:, part].astype(F32)).astype(BF16)


def join(row0, rows, pos, own, recv, half, rest, start, prev):
    piece, width = own.shape
    blk = 128
    side, steps = row0 // piece, rows // blk
    off, inner, outer = (row0 - side * piece) // blk, (row0 - start) // blk, row0 // blk
    own_spec = pl.BlockSpec((blk, width), lambda i, p: (jnp.where(p[0] == side, i + off, 0), 0))
    recv_spec = pl.BlockSpec((blk, width), lambda i, p: (jnp.where(p[0] == side, 0, i + off), 0))
    part_spec = pl.BlockSpec((blk, width), lambda i, p: (i + inner, 0))
    in_specs = [own_spec, recv_spec, part_spec, part_spec]
    args = [pos, own, recv, half, rest]
    aliases = {}
    if prev is not None:
        in_specs.append(pl.BlockSpec(memory_space=pl.ANY))
        args.append(prev)
        aliases = {5: 0}
    return pl.pallas_call(
        functools.partial(join_body, side),
        out_shape=jax.ShapeDtypeStruct((2 * piece, 2 * width), BF16),
        grid_spec=pltpu.PrefetchScalarGridSpec(
            num_scalar_prefetch=1,
            grid=(steps,),
            in_specs=in_specs,
            out_specs=pl.BlockSpec((blk, 2 * width), lambda i, p: (i + outer, 0)),
        ),
        input_output_aliases=aliases,
        cost_estimate=pl.CostEstimate(flops=rows * width, bytes_accessed=10 * rows * width, transcendentals=0),
        name="join",
    )(*args)


def solution(mesh):
    act_spec = P(("depth", "row"), None, "col")
    mat_spec = P("row", "col")
    vec_spec = P("col")
    bias_spec = P("col", None)

    def swap(val, axis):
        return lax.ppermute(val, axis, SWAP)

    def tie(val, *deps):
        return lax.optimization_barrier((val,) + deps)[0]

    def gather(val, axes):
        return lax.all_gather(val, axes, axis=0, tiled=True)

    def scatter(val, axes):
        return lax.psum_scatter(val, axes, scatter_dimension=0, tiled=True)

    def block(x, ln_g, ln_b, w_qkv, b_qkv, w_o, b_o, d_y):
        num_seq, seq, width = x.shape
        half = num_seq // 2 * seq
        tokens = num_seq * seq
        piece = w_qkv.shape[0] // 2
        hw = width // 2
        col = lax.axis_index("col")
        dep = lax.axis_index("depth")
        other = 1 - col

        def grp_s(val):
            return jnp.reshape(val, (1,)).astype(jnp.int32)

        x2 = x.reshape(tokens, width)
        dy2 = d_y.reshape(tokens, width)
        col_arr, oth_arr, dep_arr = grp_s(col), grp_s(other), grp_s(dep)
        own_grp = [grp_s(col * 2 + j) for j in range(2)]
        oth_grp = [grp_s(other * 2 + j) for j in range(2)]

        def group_cols(val, j):
            return [val[:, t * width + j * hw:t * width + (j + 1) * hw] for t in range(3)]

        def slab(j):
            part = lax.dynamic_slice_in_dim(w_qkv, dep * piece, piece, 0)
            return jnp.concatenate(group_cols(part, j), axis=1)

        def send(val, axis="col"):
            return swap(val, axis)

        nb = hw // 128
        bias = jnp.concatenate([b_qkv[(2 * t + j) * nb:(2 * t + j + 1) * nb] for j in range(2) for t in range(3)], axis=0)
        vecs = jnp.concatenate([ln_g.reshape(-1, 128), ln_b.reshape(-1, 128), b_o.reshape(-1, 128), bias], axis=0)
        rows2 = half // 2
        x_out = [lax.dynamic_slice_in_dim(x2, other * half, rows2, 0)]
        vecs = tie(vecs, x_out[0])
        vecs_r = send(vecs)
        slab_a = tie(slab(0), x_out[0])
        x_out.append(lax.dynamic_slice_in_dim(tie(x2, slab_a), other * half + rows2, rows2, 0))
        slab_b = tie(slab(1), x_out[1])
        wo_out = lax.dynamic_slice_in_dim(tie(w_o, slab_b), dep * piece, piece, 0)
        dy_out = lax.dynamic_slice_in_dim(tie(dy2, wo_out), other * half, half, 0)
        x_recv = [send(x_out[0])]
        wa_in = send(slab_a)
        x_recv.append(send(x_out[1]))
        wb_in = send(slab_b)
        wo_in = send(wo_out)
        dy_recv = send(dy_out)
        w_perm = regroup(tie(w_qkv, dy_out))
        wo_own = gather(w_o, "row")
        w_own = gather(w_perm, "row")

        nv = width // 128
        first = col == 0

        db_o = jnp.sum(dy2.astype(F32), axis=0)
        wq_oth = [None, None]
        qkv_oth = [None, None]
        dqkv_oth = [None, None]
        sum_oth = [None, None]

        def held(*vals):
            return lax.optimization_barrier(vals)

        def project(j):
            return (nn_dot(xn, wq_oth[j]) + bq_oth[j]).astype(BF16)

        def weight_grad(lhs, rhs, col0=0, cols=None):
            return weight_grad_call(lhs, rhs, col0, cols or rhs.shape[1])

        dy_own = lax.dynamic_slice_in_dim(tie(dy2, dy_out), col * half, half, 0)
        datt_part = nt_dot(tie(dy_own, w_perm), wo_own)

        vecs_r = tie(vecs_r, datt_part)

        def both(lo, hi):
            a = vecs[lo:hi].reshape(1, -1)
            b = vecs_r[lo:hi].reshape(1, -1)
            return jnp.concatenate([jnp.where(first, a, b), jnp.where(first, b, a)], axis=1)

        g_full = both(0, nv)
        b_full = both(nv, 2 * nv)
        bo_oth = vecs_r[2 * nv:3 * nv].reshape(-1)
        bq_own = bias.reshape(-1)
        bq_oth = vecs_r[3 * nv:].reshape(2, 3 * hw)

        xn, stats = ln_fwd(col_arr, tie(x2, datt_part, db_o), x_recv[0], g_full, b_full, 0, half, None)
        qkv_own = project_rows(xn, w_own, bq_own, 0, rows2, None)
        wa_in, qkv_own = held(wa_in, qkv_own)
        wq_oth[0] = gather(wa_in, ("row", "depth"))
        att = attn_fwd(own_grp[0], qkv_own, 2, hw, seq, 0, rows2, None)
        xn, stats = ln_fwd(col_arr, tie(x2, att), x_recv[1], g_full, b_full, rows2, half, (xn, stats))
        qkv_own = project_rows(xn, w_own, bq_own, rows2, rows2, qkv_own)
        att = attn_fwd(own_grp[0], qkv_own, 2, hw, seq, rows2, rows2, att)
        wb_in, xn, att = held(wb_in, xn, att)
        wq_oth[1] = gather(wb_in, ("row", "depth"))
        qkv_oth[0] = project(0)
        att = attn_fwd(oth_grp[0], qkv_oth[0], 1, hw, seq, 0, half, att)
        wo_in, att, xn = held(wo_in, att, xn)
        wo_oth = gather(wo_in, ("row", "depth"))
        y_part = out_early(col_arr, att, wo_own)
        qkv_oth[1] = (nn_dot(tie(xn, y_part), wq_oth[1]) + bq_oth[1]).astype(BF16)
        att = attn_fwd(oth_grp[1], qkv_oth[1], 1, hw, seq, 0, half, att)
        y_send, y_recv = [], []
        for i in range(2):
            part_att = (att if i == 0 else tie(att, y_send[0]))[i * rows2:(i + 1) * rows2]
            y_send.append((x_recv[i].astype(F32) + nn_dot(part_att, wo_oth) + bo_oth).astype(BF16))
            y_recv.append(send(y_send[i]))
        y = out_rows(col_arr, tie(y_part, y_send[1]), att, wo_own, x2, b_o.reshape(1, -1))

        def back_far(j, gate):
            dqkv_oth[j], sum_oth[j] = attn_bwd(oth_grp[j], tie(qkv_oth[j], gate), d_att, 0, 1, hw, seq, 0, half, None)

        def back_own(j, gate, prev):
            return attn_bwd(own_grp[j], tie(qkv_own, gate), d_att, j, 2, hw, seq, 0, half, prev)

        wide = 3 * hw
        sum_own = [None, None]
        d_att = (nt_dot(tie(dy_recv, y), wo_oth) + datt_part).astype(BF16)
        dwo_far = weight_grad(tie(att, d_att), dy_recv)
        red_of = scatter(dwo_far, "row")
        back_far(0, dwo_far)
        red_of, dqkv_oth[0] = held(red_of, dqkv_oth[0])
        far_o = send(red_of)
        dw_a = weight_grad(xn, dqkv_oth[0])
        red_a = scatter(dw_a, ("row", "depth"))
        dwo_near = weight_grad(tie(att, dw_a), dy_own)
        red_on = scatter(dwo_near, "row")
        back_far(1, dwo_near)
        dw_b = weight_grad(xn, dqkv_oth[1])
        red_b = scatter(dw_b, "row")
        red_a, dw_b = held(red_a, dw_b)
        far_a = send(red_a)
        dqkv_own, sum_own[0] = back_own(0, dw_b, None)
        far_o, red_on, dqkv_own = held(far_o, red_on, dqkv_own)
        half_o = (red_on.astype(F32) + far_o.astype(F32)).astype(BF16)
        half_r = send(half_o, "depth")
        dqkv_own = tie(dqkv_own, half_o)
        dw_oa = weight_grad(xn, dqkv_own, 0, wide)
        red_oa = scatter(dw_oa, ("row", "depth"))
        red_b, dw_oa = held(red_b, dw_oa)
        far_b = send(red_b)
        dqkv_own, sum_own[1] = back_own(1, dw_oa, dqkv_own)
        dw_ob = weight_grad(xn, dqkv_own, wide, wide)
        red_ob = scatter(dw_ob, "row")

        unit = half // 8
        parts = (2 * unit, 2 * unit, 2 * unit, unit, unit)
        cut = piece + piece // 2
        dx, gate, lo = None, dw_ob, 0
        dx_recv, sums_n = [], []
        grads = [dqkv_own, *dqkv_oth]
        for part, rows in enumerate(parts):
            grads[1] = tie(grads[1], gate)
            y_pair = (*y_recv, y) if part == 2 else None
            dx, dx_send, dg8, db8, *rest = dx_part(col_arr, grads, (w_own, *wq_oth), x2, x_recv, dy2, dy_recv, stats, g_full, lo, rows, dx, y_pair)
            y = rest[0] if rest else y
            lo += rows
            sums_n.append((dg8, db8))
            dx_recv.append(send(dx_send))
            gate = dx_send
            if part == 0:
                far_a, red_oa, gate = held(far_a, red_oa, gate)
                half_a = (red_oa.astype(F32) + far_a.astype(F32)).astype(BF16)
                rest_a = send(half_a, "depth")
                gate = half_a
            if part == 1:
                far_b, red_ob, gate = held(far_b, red_ob, gate)
                half_b, rest_b = [], []
                for i in range(2):
                    part_rows = slice(0, cut) if i == 0 else slice(cut, None)
                    half_b.append((tie(red_ob, gate)[part_rows].astype(F32) + far_b[part_rows].astype(F32)).astype(BF16))
                    rest_b.append(send(half_b[i], "depth"))
                    gate = half_b[i]

        def natural(pair):
            vals = [jnp.sum(s, axis=0).reshape(3, hw) for s in pair]
            return jnp.concatenate([vals[j][t] for t in range(3) for j in range(2)])

        dg = jnp.sum(sum(pair[0] for pair in sums_n), axis=0)
        dbn = jnp.sum(sum(pair[1] for pair in sums_n), axis=0)
        far = jnp.concatenate([natural(sum_oth), lax.dynamic_slice_in_dim(dg, other * width, width), lax.dynamic_slice_in_dim(dbn, other * width, width)])
        near = jnp.concatenate([natural(sum_own), lax.dynamic_slice_in_dim(dg, col * width, width), lax.dynamic_slice_in_dim(dbn, col * width, width)])
        near = near.reshape(-1, 128)
        far = send(far.reshape(-1, 128))
        far, gate = held(far, gate)
        total = jnp.concatenate([near + far, db_o.reshape(-1, 128)], axis=0)
        row_in = send(total, "row")
        dw_o = (tie(half_o, total).astype(F32) + half_r.astype(F32)).astype(BF16)
        row_in, dw_o = held(row_in, dw_o)
        total = total + row_in
        dep_in = send(total, "depth")
        place, lo = dw_o, 0
        for part, rows in enumerate(parts):
            if part == 3:
                dw_qkv = join(0, piece, dep_arr, half_a, tie(rest_a, dx), half_b[0], rest_b[0], 0, None)
                dw_qkv = join(piece, cut - piece, dep_arr, half_a, rest_a, half_b[0], rest_b[0], 0, dw_qkv)
                place = dw_qkv
            if part == 4:
                dw_qkv = join(cut, 2 * piece - cut, dep_arr, half_a, tie(rest_a, dx), half_b[1], rest_b[1], cut, dw_qkv)
                place = dw_qkv
            dx = lax.dynamic_update_slice(dx, tie(dx_recv[part], place), (other * half + lo, 0))
            lo += rows
        total = total + tie(dep_in, dx)
        db_o = total[-nv:]
        nq = 3 * nv
        return (
            y.reshape(x.shape),
            dx.reshape(x.shape),
            dw_qkv,
            total[:nq],
            dw_o,
            db_o.reshape(-1),
            total[nq:nq + nv].reshape(-1),
            total[nq + nv:nq + 2 * nv].reshape(-1),
        )

    return jax.shard_map(
        block,
        mesh=mesh,
        in_specs=(act_spec, vec_spec, vec_spec, mat_spec, bias_spec, mat_spec, vec_spec, act_spec),
        out_specs=(act_spec, act_spec, mat_spec, bias_spec, mat_spec, vec_spec, vec_spec, vec_spec),
        check_vma=False,
    )
```

```python
import functools

import jax
import jax.numpy as jnp
from jax import lax
from jax.experimental import pallas as pl
from jax.experimental.pallas import tpu as pltpu
from jax.sharding import PartitionSpec as P


LN_EPS = 1e-5
SWAP = [(0, 1), (1, 0)]
F32 = jnp.float32
BF16 = jnp.bfloat16
LOG2E = 1.4426950408889634


def nt_dot(lhs, rhs):
    return lax.dot_general(lhs, rhs, (((1,), (1,)), ((), ())), preferred_element_type=F32)


def tn_dot(lhs, rhs):
    return lax.dot_general(lhs, rhs, (((0,), (0,)), ((), ())), preferred_element_type=F32)


def nn_dot(lhs, rhs):
    return lax.dot_general(lhs, rhs, (((1,), (0,)), ((), ())), preferred_element_type=F32)


def row_sum(val):
    return jnp.sum(val, -1, keepdims=True)


def group_rows(i, unroll, step):
    return [pl.ds(pl.multiple_of((i * unroll + u) * step, step), step) for u in range(unroll)]


def ln_fwd_body(col_ref, own_ref, recv_ref, g_ref, b_ref, *rest):
    xn_ref, stat_ref = rest[-2:]
    width = own_ref.shape[1]
    inv_n = 1.0 / (2 * width)
    col = col_ref[0]
    own_cols = pl.ds(pl.multiple_of(col * width, width), width)
    far_cols = pl.ds(pl.multiple_of((1 - col) * width, width), width)
    step, unroll = 16, 4

    @pl.loop(0, own_ref.shape[0] // (step * unroll))
    def _(i):
        groups = group_rows(i, unroll, step)
        means = [row_sum(own_ref[r, :].astype(F32) + recv_ref[r, :].astype(F32)) * inv_n for r in groups]
        invs = []
        for r, mean in zip(groups, means):
            own = own_ref[r, :].astype(F32) - mean
            far = recv_ref[r, :].astype(F32) - mean
            invs.append(lax.rsqrt(row_sum(own * own + far * far) * inv_n + LN_EPS))
        for r, mean, inv in zip(groups, means, invs):
            stat_ref[r, :128] = jnp.broadcast_to(mean, (step, 128))
            stat_ref[r, 128:] = jnp.broadcast_to(inv, (step, 128))
            for src, cols in ((own_ref, own_cols), (recv_ref, far_cols)):
                hat = (src[r, :].astype(F32) - mean) * inv
                xn_ref[r, cols] = (hat * g_ref[:, cols] + b_ref[:, cols]).astype(BF16)


def ln_fwd(col, x_loc, x_recv, g_full, b_full, row0, total, prev):
    rows, width = x_recv.shape
    blk = 256
    nall = total // blk
    off = row0 // blk
    in_specs = [
        pl.BlockSpec((blk, width), lambda i, c: (i + off + c[0] * nall, 0)),
        pl.BlockSpec((blk, width), lambda i, c: (i, 0)),
        pl.BlockSpec((1, 2 * width), lambda i, c: (0, 0)),
        pl.BlockSpec((1, 2 * width), lambda i, c: (0, 0)),
    ]
    args = [col, x_loc, x_recv, g_full, b_full]
    aliases = {}
    if prev is not None:
        in_specs.extend([pl.BlockSpec(memory_space=pl.ANY)] * 2)
        args.extend(prev)
        aliases = {5: 0, 6: 1}
    return pl.pallas_call(
        ln_fwd_body,
        out_shape=(jax.ShapeDtypeStruct((total, 2 * width), BF16), jax.ShapeDtypeStruct((total, 256), F32)),
        grid_spec=pltpu.PrefetchScalarGridSpec(
            num_scalar_prefetch=1,
            grid=(rows // blk,),
            in_specs=in_specs,
            out_specs=(pl.BlockSpec((blk, 2 * width), lambda i, c: (i + off, 0)), pl.BlockSpec((blk, 256), lambda i, c: (i + off, 0))),
        ),
        input_output_aliases=aliases,
        cost_estimate=pl.CostEstimate(flops=20 * rows * 2 * width, bytes_accessed=8 * rows * width, transcendentals=0),
        name="ln_fwd",
    )(*args)


def ln_bwd_rows(dxn_ref, sides, stat_ref, g_ref, dg_ref, db_ref):
    rows = dxn_ref.shape[0]
    inv_n = 1.0 / dxn_ref.shape[1]
    step, unroll = 16, 4

    def fold(val):
        return jnp.sum(val.reshape(val.shape[0] // 8, 8, val.shape[1]), axis=0)

    @pl.loop(0, rows // (step * unroll))
    def _(i):
        groups = group_rows(i, unroll, step)
        full = []
        for r in groups:
            mean, inv = stat_ref[r, 0:1], stat_ref[r, 128:129]
            m1, m2 = 0.0, 0.0
            for x_ref, _, _, cols in sides:
                part = dxn_ref[r, cols] * g_ref[:, cols]
                m1 = m1 + part
                m2 = m2 + part * (x_ref[r, :].astype(F32) - mean)
            full.append((mean, inv, row_sum(m1) * inv_n, row_sum(m2) * inv_n * inv))
        for x_ref, dy_ref, dx_ref, cols in sides:
            sum_g = sum_b = None
            for r, (mean, inv, m1, m2) in zip(groups, full):
                hat = (x_ref[r, :].astype(F32) - mean) * inv
                d = dxn_ref[r, cols]
                add_g, add_b = fold(d * hat), fold(d)
                sum_g = add_g if sum_g is None else sum_g + add_g
                sum_b = add_b if sum_b is None else sum_b + add_b
                dx_ref[r, :] = (dy_ref[r, :].astype(F32) + inv * (d * g_ref[:, cols] - m1 - hat * m2)).astype(BF16)
            dg_ref[:, cols] += sum_g
            db_ref[:, cols] += sum_b


def dx_body(row0, half, steps, with_y, col_ref, d_own, d_a, d_b, w_own, w_a, w_b, x_ref, x0_ref, x1_ref, dy_ref, dyr_ref, stat_ref, g_ref, *rest):
    if with_y:
        yr0_ref, yr1_ref, y_ref, y_buf, y_sems = rest[-16], rest[-15], rest[-9], rest[-2], rest[-1]
        rest = rest[:-9] + rest[-8:-2]
    dx_ref, send_ref, dg_ref, db_ref, acc, w_buf, d_buf, ln_buf, sems, ln_sems = rest[-10:]
    m = pl.program_id(0)
    blk, wide = d_buf.shape[1:]
    width = x_ref.shape[1]
    col = col_ref[0]
    sources, count = [], 0
    for d, w in ((d_own, w_own), (d_a, w_a), (d_b, w_b)):
        chunks = d.shape[1] // wide
        sources.append((d, w, count, chunks))
        count += chunks

    def copies(d, w, block, chunk, slot):
        rows = pl.ds(pl.multiple_of(row0 + block * blk, blk), blk)
        cols = pl.ds(pl.multiple_of(chunk * wide, wide), wide)
        return (
            pltpu.make_async_copy(w.at[:, cols], w_buf.at[slot], sems.at[0, slot]),
            pltpu.make_async_copy(d.at[rows, cols], d_buf.at[slot], sems.at[1, slot]),
        )

    def fetch(block, chunk, slot):
        for d, w, lo, chunks in sources:
            @pl.when((chunk >= lo) & (chunk < lo + chunks))
            def _():
                for copy in copies(d, w, block, chunk - lo, slot):
                    copy.start()

    @pl.when(m == 0)
    def _():
        dg_ref[...] = jnp.zeros_like(dg_ref)
        db_ref[...] = jnp.zeros_like(db_ref)
        fetch(0, 0, 0)

    row = row0 + m * blk
    own_rows = pl.ds(pl.multiple_of(col * half + row, blk), blk)
    far_rows = pl.ds(pl.multiple_of(row, blk), blk)
    pair = half // 2
    x0_rows = pl.ds(pl.multiple_of(jnp.minimum(row, pair - blk), blk), blk)
    x1_rows = pl.ds(pl.multiple_of(jnp.maximum(row - pair, 0), blk), blk)

    def ln_copy(i, src):
        return pltpu.make_async_copy(src, ln_buf.at[i], ln_sems.at[i])

    ln_copy(0, x_ref.at[own_rows]).start()
    ln_copy(2, dy_ref.at[own_rows]).start()
    ln_copy(3, dyr_ref.at[far_rows]).start()

    @pl.when(row < pair)
    def _():
        ln_copy(1, x0_ref.at[x0_rows]).start()

    @pl.when(row >= pair)
    def _():
        ln_copy(1, x1_ref.at[x1_rows]).start()

    acc[...] = jnp.zeros_like(acc)

    y_blocks = steps * count // 2
    y_rows = half // (2 * y_blocks)

    def y_in(t, src, block):
        place = pl.ds(pl.multiple_of(block * y_rows, y_rows), y_rows)
        return pltpu.make_async_copy(src.at[place], y_buf.at[lax.rem(t, 2)], y_sems.at[0, lax.rem(t, 2)])

    def y_out(t):
        place = pl.ds(pl.multiple_of((1 - col) * half + t * y_rows, y_rows), y_rows)
        return pltpu.make_async_copy(y_buf.at[lax.rem(t, 2)], y_ref.at[place], y_sems.at[1, lax.rem(t, 2)])

    @pl.loop(0, count)
    def _(k):
        t = m * count + k
        slot = lax.rem(t, 2)
        if with_y:
            @pl.when(t >= 2)
            def _():
                y_out(t - 2).wait()

            @pl.when(t < y_blocks)
            def _():
                y_in(t, yr0_ref, jnp.minimum(t, y_blocks - 1)).start()

            @pl.when(t >= y_blocks)
            def _():
                y_in(t, yr1_ref, jnp.maximum(t - y_blocks, 0)).start()

            @pl.when(t >= 1)
            def _():
                y_in(t - 1, yr0_ref, 0).wait()
                y_out(t - 1).start()

        @pl.when(k + 1 < count)
        def _():
            fetch(m, k + 1, 1 - slot)

        @pl.when((k + 1 == count) & (m + 1 < steps))
        def _():
            fetch(m + 1, 0, 1 - slot)

        for copy in copies(d_a, w_a, 0, 0, slot):
            copy.wait()
        acc[...] += nt_dot(d_buf[slot], w_buf[slot])

    for i in range(4):
        ln_copy(i, dyr_ref.at[far_rows]).wait()
    if with_y:
        @pl.when(m == steps - 1)
        def _():
            last = steps * count - 1
            y_in(last, yr0_ref, 0).wait()
            y_out(last).start()
            y_out(last - 1).wait()
            y_out(last).wait()

    own_cols = pl.ds(pl.multiple_of(col * width, width), width)
    far_cols = pl.ds(pl.multiple_of((1 - col) * width, width), width)
    sides = ((ln_buf.at[0], ln_buf.at[2], dx_ref, own_cols), (ln_buf.at[1], ln_buf.at[3], send_ref, far_cols))
    ln_bwd_rows(acc, sides, stat_ref, g_ref, dg_ref, db_ref)


def dx_part(col, dqkv, weights, x_loc, x_recv, dy_loc, dy_recv, stats, g_full, row0, rows, dx_prev, y_pair=None):
    total, width = dy_recv.shape
    blk, wide = 384, 1024
    off = row0 // blk
    nall = total // blk
    own_spec = pl.BlockSpec((blk, width), lambda i, c: (i + off + c[0] * nall, 0))
    sums_spec = pl.BlockSpec((8, 2 * width), lambda i, c: (0, 0))
    any_spec = pl.BlockSpec(memory_space=pl.ANY)
    in_specs = [any_spec] * 11 + [pl.BlockSpec((blk, 256), lambda i, c: (i + off, 0)), pl.BlockSpec((1, 2 * width), lambda i, c: (0, 0))]
    args = [col, *dqkv, *weights, x_loc, *x_recv, dy_loc, dy_recv, stats, g_full]
    aliases = {}
    if dx_prev is not None:
        in_specs.append(any_spec)
        args.append(dx_prev)
        aliases = {14: 0}
    out_shape = [
        jax.ShapeDtypeStruct((2 * total, width), BF16),
        jax.ShapeDtypeStruct((rows, width), BF16),
        jax.ShapeDtypeStruct((8, 2 * width), F32),
        jax.ShapeDtypeStruct((8, 2 * width), F32),
    ]
    out_specs = [own_spec, pl.BlockSpec((blk, width), lambda i, c: (i, 0)), sums_spec, sums_spec]
    scratch = [
        pltpu.VMEM((blk, 2 * width), F32),
        pltpu.VMEM((2, 2 * width, wide), BF16),
        pltpu.VMEM((2, blk, wide), BF16),
        pltpu.VMEM((4, blk, width), BF16),
        pltpu.SemaphoreType.DMA((2, 2)),
        pltpu.SemaphoreType.DMA((4,)),
    ]
    depth = sum(d.shape[1] for d in dqkv)
    if y_pair is not None:
        in_specs.extend([any_spec] * 3)
        args.extend(y_pair)
        aliases[len(args) - 1] = 4
        out_shape.append(jax.ShapeDtypeStruct(y_pair[2].shape, BF16))
        out_specs.append(any_spec)
        scratch.extend([pltpu.VMEM((2, total * blk * wide // (rows * depth), width), BF16), pltpu.SemaphoreType.DMA((2, 2))])
    return pl.pallas_call(
        functools.partial(dx_body, row0, total, rows // blk, y_pair is not None),
        out_shape=out_shape,
        grid_spec=pltpu.PrefetchScalarGridSpec(num_scalar_prefetch=1, grid=(rows // blk,), in_specs=in_specs, out_specs=out_specs, scratch_shapes=scratch),
        input_output_aliases=aliases,
        compiler_params=pltpu.CompilerParams(vmem_limit_bytes=60 * 1024 * 1024),
        cost_estimate=pl.CostEstimate(flops=4 * rows * width * depth, bytes_accessed=(rows // blk) * 4 * width * depth, transcendentals=0),
        name="dx_part",
    )(*args)


def attn_fwd_body(heads, scale, grp_ref, q_ref, k_ref, v_ref, *rest):
    out_ref = rest[-1]
    half = q_ref.shape[0] // 2
    causal = lax.broadcasted_iota(jnp.int32, (half, half), 0) >= lax.broadcasted_iota(jnp.int32, (half, half), 1)
    unroll = 8
    coef = scale * LOG2E

    @pl.loop(0, heads // unroll)
    def _(i):
        scores = []
        for j in range(unroll):
            cols = pl.ds(pl.multiple_of((i * unroll + j) * 128, 128), 128)
            k = k_ref[:, cols]
            scores.append((cols, nt_dot(q_ref[:half, cols], k[:half]), nt_dot(q_ref[half:, cols], k)))
        probs = []
        for cols, s0, s1 in scores:
            sa = jnp.where(causal, s0, -1e30)
            ea = jnp.exp2((sa - jnp.max(sa, -1, keepdims=True)) * coef)
            pa = (ea * (1.0 / row_sum(ea))).astype(BF16)
            sb, sc = s1[:, :half], jnp.where(causal, s1[:, half:], -1e30)
            top = jnp.max(jnp.maximum(sb, sc), -1, keepdims=True)
            eb, ec = jnp.exp2((sb - top) * coef), jnp.exp2((sc - top) * coef)
            inv = 1.0 / row_sum(eb + ec)
            probs.append((cols, pa, jnp.concatenate([(eb * inv).astype(BF16), (ec * inv).astype(BF16)], axis=1)))
        for cols, p0, p1 in probs:
            v = v_ref[:, cols]
            out_ref[:half, cols] = nn_dot(p0, v[:half]).astype(BF16)
            out_ref[half:, cols] = nn_dot(p1, v).astype(BF16)


def attn_fwd(grp, qkv, groups, width, seq, row0, rows, prev):
    heads = width // 128
    off = row0 // seq
    in_specs = [pl.BlockSpec((seq, width), lambda g, i, c, j=j: (i + off, 3 * g + j)) for j in range(3)]
    args = [grp, qkv, qkv, qkv]
    aliases = {}
    if prev is not None:
        in_specs.append(pl.BlockSpec(memory_space=pl.ANY))
        args.append(prev)
        aliases = {4: 0}
    nheads = rows // seq * heads * groups
    return pl.pallas_call(
        functools.partial(attn_fwd_body, heads, 128 ** -0.5),
        out_shape=jax.ShapeDtypeStruct((qkv.shape[0], 4096), BF16),
        grid_spec=pltpu.PrefetchScalarGridSpec(
            num_scalar_prefetch=1,
            grid=(groups, rows // seq),
            in_specs=in_specs,
            out_specs=pl.BlockSpec((seq, width), lambda g, i, c: (i + off, c[0] + g)),
        ),
        input_output_aliases=aliases,
        cost_estimate=pl.CostEstimate(flops=nheads * seq * seq * 128 * 8, bytes_accessed=8 * rows * width * groups, transcendentals=nheads * seq * seq),
        name="attn_fwd",
    )(*args)


def attn_bwd_body(heads, seq, scale, grp_ref, q_ref, k_ref, v_ref, d_ref, *rest):
    dq_ref, sum_ref = rest[-2:]
    width = q_ref.shape[1]
    half = seq // 2
    lanes = heads * (q_ref.shape[0] // seq)
    causal = lax.broadcasted_iota(jnp.int32, (half, half), 1) >= lax.broadcasted_iota(jnp.int32, (half, half), 0)
    coef = scale * LOG2E

    @pl.when(pl.program_id(0) == 0)
    def _():
        sum_ref[...] = jnp.zeros_like(sum_ref)

    def col_sum(val):
        return jnp.sum(val, 0, keepdims=True)

    def emit(top, bottom, start, row):
        cols = pl.ds(start, 128)
        dq_ref[row:row + half, cols] = top.astype(BF16)
        dq_ref[row + half:row + seq, cols] = bottom.astype(BF16)
        sum_ref[:, cols] += jnp.sum((top + bottom).reshape(half // 8, 8, 128), axis=0)

    first = []
    for lane in range(lanes):
        h, row = lane % heads * 128, lane // heads * seq
        rows, cols = pl.ds(row, seq), pl.ds(h, 128)
        q, k, v, d = q_ref[rows, cols], k_ref[rows, cols], v_ref[rows, cols], d_ref[rows, cols]
        first.append((h, row, nt_dot(k[:half], q), nt_dot(k[half:], q[half:]), nt_dot(v[:half], d), nt_dot(v[half:], d[half:])))
    second = []
    for h, row, s0, s1, dp0, dpc in first:
        sa = jnp.where(causal, s0[:, :half], -1e30)
        ea = jnp.exp2((sa - jnp.max(sa, 0, keepdims=True)) * coef)
        pa = ea * (1.0 / col_sum(ea))
        dpa, dpb = dp0[:, :half], dp0[:, half:]
        dsa = (pa * (dpa - col_sum(dpa * pa)) * scale).astype(BF16)
        sb, sc = s0[:, half:], jnp.where(causal, s1, -1e30)
        top = jnp.max(jnp.maximum(sb, sc), 0, keepdims=True)
        eb, ec = jnp.exp2((sb - top) * coef), jnp.exp2((sc - top) * coef)
        inv = 1.0 / col_sum(eb + ec)
        pb, pc = eb * inv, ec * inv
        dot = col_sum(dpb * pb + dpc * pc)
        dsb = (pb * (dpb - dot) * scale).astype(BF16)
        dsc = (pc * (dpc - dot) * scale).astype(BF16)
        p0 = jnp.concatenate([pa.astype(BF16), pb.astype(BF16)], axis=1)
        second.append((h, row, p0, pc.astype(BF16), dsa, dsb, dsc))
    for h, row, p0, p1, dsa, dsb, dsc in second:
        rows, cols = pl.ds(row, seq), pl.ds(h, 128)
        q, k, d = q_ref[rows, cols], k_ref[rows, cols], d_ref[rows, cols]
        emit(nn_dot(p0, d), nn_dot(p1, d[half:]), h + 2 * width, row)
        emit(nn_dot(jnp.concatenate([dsa, dsb], axis=1), q), nn_dot(dsc, q[half:]), h + width, row)
        emit(tn_dot(dsa, k[:half]), tn_dot(jnp.concatenate([dsb, dsc], axis=0), k), h, row)


def attn_bwd(grp, qkv, d_att, group, out_groups, width, seq, row0, total, prev):
    rows = qkv.shape[0]
    blk = 2 * seq
    heads = width // 128
    off = row0 // blk
    in_specs = [pl.BlockSpec((blk, width), lambda i, c, j=j: (i, 3 * group + j)) for j in range(3)]
    in_specs.append(pl.BlockSpec((blk, width), lambda i, c: (i + off, c[0])))
    args = [grp, qkv, qkv, qkv, d_att]
    aliases = {}
    if prev is not None:
        in_specs.append(pl.BlockSpec(memory_space=pl.ANY))
        args.append(prev)
        aliases = {5: 0}
    nheads = rows // seq * heads
    return pl.pallas_call(
        functools.partial(attn_bwd_body, heads, seq, 128 ** -0.5),
        out_shape=(
            jax.ShapeDtypeStruct((total, 3 * width * out_groups), BF16),
            jax.ShapeDtypeStruct((8, 3 * width), F32),
        ),
        grid_spec=pltpu.PrefetchScalarGridSpec(
            num_scalar_prefetch=1,
            grid=(rows // blk,),
            in_specs=in_specs,
            out_specs=(
                pl.BlockSpec((blk, 3 * width), lambda i, c: (i + off, group)),
                pl.BlockSpec((8, 3 * width), lambda i, c: (0, 0)),
            ),
        ),
        input_output_aliases=aliases,
        cost_estimate=pl.CostEstimate(flops=nheads * seq * seq * 128 * 20, bytes_accessed=14 * rows * width, transcendentals=nheads * seq * seq),
        name="attn_bwd",
    )(*args)


def out_early_body(col_ref, a0_ref, a1_ref, a2_ref, w0_ref, w1_ref, w2_ref, out_ref):
    part = nn_dot(a0_ref[...], w0_ref[...]) + nn_dot(a1_ref[...], w1_ref[...])
    out_ref[...] = part + nn_dot(a2_ref[...], w2_ref[...])


def out_early(col, att, w_o):
    tokens = att.shape[0]
    full, width = w_o.shape
    blk = 1024

    def group(k, c):
        return 2 * c[0] + k if k < 2 else 2 * (1 - c[0])

    return pl.pallas_call(
        out_early_body,
        out_shape=jax.ShapeDtypeStruct((tokens, width), F32),
        grid_spec=pltpu.PrefetchScalarGridSpec(
            num_scalar_prefetch=1,
            grid=(width // blk, tokens // blk),
            in_specs=[
                *[pl.BlockSpec((blk, blk), lambda n, m, c, k=k: (m, group(k, c))) for k in range(3)],
                *[pl.BlockSpec((blk, blk), lambda n, m, c, k=k: (group(k, c), n)) for k in range(3)],
            ],
            out_specs=pl.BlockSpec((blk, blk), lambda n, m, c: (m, n)),
        ),
        compiler_params=pltpu.CompilerParams(vmem_limit_bytes=56 * 1024 * 1024),
        cost_estimate=pl.CostEstimate(flops=6 * tokens * blk * width, bytes_accessed=6 * tokens * full, transcendentals=0),
        name="out_early",
    )(col, att, att, att, w_o, w_o, w_o)


def out_body(col_ref, part_ref, att_ref, w_ref, x_ref, b_ref, out_ref):
    out_ref[...] = (x_ref[...].astype(F32) + (part_ref[...] + nn_dot(att_ref[...], w_ref[...])) + b_ref[...]).astype(BF16)


def out_rows(col, part, att, w_o, x_loc, bias):
    tokens, width = part.shape
    blk = 1024
    nblk = tokens // blk
    place = pl.BlockSpec((blk, blk), lambda n, m, c: (m + c[0] * nblk, n))
    return pl.pallas_call(
        out_body,
        out_shape=jax.ShapeDtypeStruct((2 * tokens, width), BF16),
        grid_spec=pltpu.PrefetchScalarGridSpec(
            num_scalar_prefetch=1,
            grid=(width // blk, nblk),
            in_specs=[
                pl.BlockSpec((blk, blk), lambda n, m, c: (m, n)),
                pl.BlockSpec((blk, blk), lambda n, m, c: (m, 2 * (1 - c[0]) + 1)),
                pl.BlockSpec((blk, blk), lambda n, m, c: (2 * (1 - c[0]) + 1, n)),
                place,
                pl.BlockSpec((1, blk), lambda n, m, c: (0, n)),
            ],
            out_specs=place,
        ),
        compiler_params=pltpu.CompilerParams(vmem_limit_bytes=56 * 1024 * 1024),
        cost_estimate=pl.CostEstimate(flops=2 * tokens * blk * width, bytes_accessed=12 * tokens * width, transcendentals=0),
        name="out_rows",
    )(col, part, att, w_o, x_loc, bias)


def weight_grad_body(lhs_ref, rhs_ref, out_ref):
    out_ref[...] = tn_dot(lhs_ref[...], rhs_ref[...]).astype(BF16)


def weight_grad_call(lhs, rhs, col0, cols):
    tokens, full = lhs.shape
    blk = 1024
    off = col0 // blk
    return pl.pallas_call(
        weight_grad_body,
        out_shape=jax.ShapeDtypeStruct((full, cols), BF16),
        grid=(cols // blk, full // blk),
        in_specs=[pl.BlockSpec((tokens, blk), lambda n, m: (0, m)), pl.BlockSpec((tokens, blk), lambda n, m: (0, n + off))],
        out_specs=pl.BlockSpec((blk, blk), lambda n, m: (m, n)),
        compiler_params=pltpu.CompilerParams(vmem_limit_bytes=56 * 1024 * 1024),
        cost_estimate=pl.CostEstimate(flops=2 * tokens * full * cols, bytes_accessed=4 * tokens * full, transcendentals=0),
        name="weight_grad",
    )(lhs, rhs)


def project_body(xn_ref, w_ref, b_ref, *rest):
    rest[-1][...] = (nn_dot(xn_ref[...], w_ref[...]) + b_ref[...]).astype(BF16)


def project_rows(xn, w, bias, row0, rows, prev):
    total, full = xn.shape
    width = w.shape[1]
    blk, wide = 768, 1024
    off = row0 // blk
    in_specs = [
        pl.BlockSpec((blk, full), lambda n, m: (m + off, 0)),
        pl.BlockSpec((full, wide), lambda n, m: (0, n)),
        pl.BlockSpec((1, wide), lambda n, m: (0, n)),
    ]
    args = [xn, w, bias.reshape(1, -1)]
    aliases = {}
    if prev is not None:
        in_specs.append(pl.BlockSpec(memory_space=pl.ANY))
        args.append(prev)
        aliases = {3: 0}
    return pl.pallas_call(
        project_body,
        out_shape=jax.ShapeDtypeStruct((total, width), BF16),
        grid=(width // wide, rows // blk),
        in_specs=in_specs,
        out_specs=pl.BlockSpec((blk, wide), lambda n, m: (m + off, n)),
        input_output_aliases=aliases,
        compiler_params=pltpu.CompilerParams(vmem_limit_bytes=56 * 1024 * 1024),
        cost_estimate=pl.CostEstimate(flops=2 * rows * full * width, bytes_accessed=2 * full * width, transcendentals=0),
        name="project",
    )(*args)


def regroup_body(src_ref, out_ref):
    wide = src_ref.shape[1] // 6
    for j in range(2):
        for t in range(3):
            out_ref[:, (3 * j + t) * wide:(3 * j + t + 1) * wide] = src_ref[:, (2 * t + j) * wide:(2 * t + j + 1) * wide]


def regroup(val):
    rows, width = val.shape
    spec = pl.BlockSpec((256, width), lambda i: (i, 0))
    return pl.pallas_call(
        regroup_body,
        out_shape=jax.ShapeDtypeStruct(val.shape, val.dtype),
        grid=(rows // 256,),
        in_specs=[spec],
        out_specs=spec,
        cost_estimate=pl.CostEstimate(flops=rows * width, bytes_accessed=4 * rows * width, transcendentals=0),
        name="regroup",
    )(val)


def join_body(side, pos_ref, own_ref, recv_ref, half_ref, rest_ref, *rest):
    out_ref = rest[-1]
    wide = own_ref.shape[1] // 3
    mine = pos_ref[0] == side

    def cols(t, j):
        return pl.ds((2 * t + j) * wide, wide)

    for src, flag in ((own_ref, mine), (recv_ref, jnp.logical_not(mine))):
        @pl.when(flag)
        def _(src=src):
            for t in range(3):
                out_ref[:, cols(t, 0)] = src[:, t * wide:(t + 1) * wide]

    for t in range(3):
        part = pl.ds(t * wide, wide)
        out_ref[:, cols(t, 1)] = (half_ref[:, part].astype(F32) + rest_ref[:, part].astype(F32)).astype(BF16)


def join(row0, rows, pos, own, recv, half, rest, start, prev):
    piece, width = own.shape
    blk = 128
    side, steps = row0 // piece, rows // blk
    off, inner, outer = (row0 - side * piece) // blk, (row0 - start) // blk, row0 // blk
    own_spec = pl.BlockSpec((blk, width), lambda i, p: (jnp.where(p[0] == side, i + off, 0), 0))
    recv_spec = pl.BlockSpec((blk, width), lambda i, p: (jnp.where(p[0] == side, 0, i + off), 0))
    part_spec = pl.BlockSpec((blk, width), lambda i, p: (i + inner, 0))
    in_specs = [own_spec, recv_spec, part_spec, part_spec]
    args = [pos, own, recv, half, rest]
    aliases = {}
    if prev is not None:
        in_specs.append(pl.BlockSpec(memory_space=pl.ANY))
        args.append(prev)
        aliases = {5: 0}
    return pl.pallas_call(
        functools.partial(join_body, side),
        out_shape=jax.ShapeDtypeStruct((2 * piece, 2 * width), BF16),
        grid_spec=pltpu.PrefetchScalarGridSpec(
            num_scalar_prefetch=1,
            grid=(steps,),
            in_specs=in_specs,
            out_specs=pl.BlockSpec((blk, 2 * width), lambda i, p: (i + outer, 0)),
        ),
        input_output_aliases=aliases,
        cost_estimate=pl.CostEstimate(flops=rows * width, bytes_accessed=10 * rows * width, transcendentals=0),
        name="join",
    )(*args)


def solution(mesh):
    act_spec = P(("depth", "row"), None, "col")
    mat_spec = P("row", "col")
    vec_spec = P("col")
    bias_spec = P("col", None)

    def swap(val, axis):
        return lax.ppermute(val, axis, SWAP)

    def tie(val, *deps):
        return lax.optimization_barrier((val,) + deps)[0]

    def gather(val, axes):
        return lax.all_gather(val, axes, axis=0, tiled=True)

    def scatter(val, axes):
        return lax.psum_scatter(val, axes, scatter_dimension=0, tiled=True)

    def block(x, ln_g, ln_b, w_qkv, b_qkv, w_o, b_o, d_y):
        num_seq, seq, width = x.shape
        half = num_seq // 2 * seq
        tokens = num_seq * seq
        piece = w_qkv.shape[0] // 2
        hw = width // 2
        col = lax.axis_index("col")
        dep = lax.axis_index("depth")
        other = 1 - col

        def grp_s(val):
            return jnp.reshape(val, (1,)).astype(jnp.int32)

        x2 = x.reshape(tokens, width)
        dy2 = d_y.reshape(tokens, width)
        col_arr, oth_arr, dep_arr = grp_s(col), grp_s(other), grp_s(dep)
        own_grp = [grp_s(col * 2 + j) for j in range(2)]
        oth_grp = [grp_s(other * 2 + j) for j in range(2)]

        def group_cols(val, j):
            return [val[:, t * width + j * hw:t * width + (j + 1) * hw] for t in range(3)]

        def slab(j):
            part = lax.dynamic_slice_in_dim(w_qkv, dep * piece, piece, 0)
            return jnp.concatenate(group_cols(part, j), axis=1)

        def send(val, axis="col"):
            return swap(val, axis)

        nb = hw // 128
        bias = jnp.concatenate([b_qkv[(2 * t + j) * nb:(2 * t + j + 1) * nb] for j in range(2) for t in range(3)], axis=0)
        vecs = jnp.concatenate([ln_g.reshape(-1, 128), ln_b.reshape(-1, 128), b_o.reshape(-1, 128), bias], axis=0)
        rows2 = half // 2
        x_out = [lax.dynamic_slice_in_dim(x2, other * half, rows2, 0)]
        vecs = tie(vecs, x_out[0])
        vecs_r = send(vecs)
        slab_a = tie(slab(0), x_out[0])
        x_out.append(lax.dynamic_slice_in_dim(tie(x2, slab_a), other * half + rows2, rows2, 0))
        slab_b = tie(slab(1), x_out[1])
        wo_out = lax.dynamic_slice_in_dim(tie(w_o, slab_b), dep * piece, piece, 0)
        dy_out = lax.dynamic_slice_in_dim(tie(dy2, wo_out), other * half, half, 0)
        x_recv = [send(x_out[0])]
        wa_in = send(slab_a)
        x_recv.append(send(x_out[1]))
        wb_in = send(slab_b)
        wo_in = send(wo_out)
        dy_recv = send(dy_out)
        w_perm = regroup(tie(w_qkv, dy_out))
        wo_own = gather(w_o, "row")
        w_own = gather(w_perm, "row")

        nv = width // 128
        first = col == 0

        db_o = jnp.sum(dy2.astype(F32), axis=0)
        wq_oth = [None, None]
        qkv_oth = [None, None]
        dqkv_oth = [None, None]
        sum_oth = [None, None]

        def held(*vals):
            return lax.optimization_barrier(vals)

        def project(j):
            return (nn_dot(xn, wq_oth[j]) + bq_oth[j]).astype(BF16)

        def weight_grad(lhs, rhs, col0=0, cols=None):
            return weight_grad_call(lhs, rhs, col0, cols or rhs.shape[1])

        dy_own = lax.dynamic_slice_in_dim(tie(dy2, dy_out), col * half, half, 0)
        datt_part = nt_dot(tie(dy_own, w_perm), wo_own)

        vecs_r = tie(vecs_r, datt_part)

        def both(lo, hi):
            a = vecs[lo:hi].reshape(1, -1)
            b = vecs_r[lo:hi].reshape(1, -1)
            return jnp.concatenate([jnp.where(first, a, b), jnp.where(first, b, a)], axis=1)

        g_full = both(0, nv)
        b_full = both(nv, 2 * nv)
        bo_oth = vecs_r[2 * nv:3 * nv].reshape(-1)
        bq_own = bias.reshape(-1)
        bq_oth = vecs_r[3 * nv:].reshape(2, 3 * hw)

        xn, stats = ln_fwd(col_arr, tie(x2, datt_part, db_o), x_recv[0], g_full, b_full, 0, half, None)
        qkv_own = project_rows(xn, w_own, bq_own, 0, rows2, None)
        wa_in, qkv_own = held(wa_in, qkv_own)
        wq_oth[0] = gather(wa_in, ("row", "depth"))
        att = attn_fwd(own_grp[0], qkv_own, 2, hw, seq, 0, rows2, None)
        xn, stats = ln_fwd(col_arr, tie(x2, att), x_recv[1], g_full, b_full, rows2, half, (xn, stats))
        qkv_own = project_rows(xn, w_own, bq_own, rows2, rows2, qkv_own)
        att = attn_fwd(own_grp[0], qkv_own, 2, hw, seq, rows2, rows2, att)
        wb_in, xn, att = held(wb_in, xn, att)
        wq_oth[1] = gather(wb_in, ("row", "depth"))
        qkv_oth[0] = project(0)
        att = attn_fwd(oth_grp[0], qkv_oth[0], 1, hw, seq, 0, half, att)
        wo_in, att, xn = held(wo_in, att, xn)
        wo_oth = gather(wo_in, ("row", "depth"))
        y_part = out_early(col_arr, att, wo_own)
        qkv_oth[1] = (nn_dot(tie(xn, y_part), wq_oth[1]) + bq_oth[1]).astype(BF16)
        att = attn_fwd(oth_grp[1], qkv_oth[1], 1, hw, seq, 0, half, att)
        y_send, y_recv = [], []
        for i in range(2):
            part_att = (att if i == 0 else tie(att, y_send[0]))[i * rows2:(i + 1) * rows2]
            y_send.append((x_recv[i].astype(F32) + nn_dot(part_att, wo_oth) + bo_oth).astype(BF16))
            y_recv.append(send(y_send[i]))
        y = out_rows(col_arr, tie(y_part, y_send[1]), att, wo_own, x2, b_o.reshape(1, -1))

        def back_far(j, gate):
            dqkv_oth[j], sum_oth[j] = attn_bwd(oth_grp[j], tie(qkv_oth[j], gate), d_att, 0, 1, hw, seq, 0, half, None)

        def back_own(j, gate, prev):
            return attn_bwd(own_grp[j], tie(qkv_own, gate), d_att, j, 2, hw, seq, 0, half, prev)

        wide = 3 * hw
        sum_own = [None, None]
        d_att = (nt_dot(tie(dy_recv, y), wo_oth) + datt_part).astype(BF16)
        dwo_far = weight_grad(tie(att, d_att), dy_recv)
        red_of = scatter(dwo_far, "row")
        back_far(0, dwo_far)
        red_of, dqkv_oth[0] = held(red_of, dqkv_oth[0])
        far_o = send(red_of)
        dw_a = weight_grad(xn, dqkv_oth[0])
        red_a = scatter(dw_a, ("row", "depth"))
        dwo_near = weight_grad(tie(att, dw_a), dy_own)
        red_on = scatter(dwo_near, "row")
        back_far(1, dwo_near)
        dw_b = weight_grad(xn, dqkv_oth[1])
        red_b = scatter(dw_b, "row")
        red_a, dw_b = held(red_a, dw_b)
        far_a = send(red_a)
        dqkv_own, sum_own[0] = back_own(0, dw_b, None)
        far_o, red_on, dqkv_own = held(far_o, red_on, dqkv_own)
        half_o = (red_on.astype(F32) + far_o.astype(F32)).astype(BF16)
        half_r = send(half_o, "depth")
        dqkv_own = tie(dqkv_own, half_o)
        dw_oa = weight_grad(xn, dqkv_own, 0, wide)
        red_oa = scatter(dw_oa, ("row", "depth"))
        red_b, dw_oa = held(red_b, dw_oa)
        far_b = send(red_b)
        dqkv_own, sum_own[1] = back_own(1, dw_oa, dqkv_own)
        dw_ob = weight_grad(xn, dqkv_own, wide, wide)
        red_ob = scatter(dw_ob, "row")

        unit = half // 8
        parts = (2 * unit, 2 * unit, 2 * unit, unit, unit)
        cut = piece + 3 * piece // 4
        dx, gate, lo = None, dw_ob, 0
        dx_recv, sums_n = [], []
        grads = [dqkv_own, *dqkv_oth]
        for part, rows in enumerate(parts):
            grads[1] = tie(grads[1], gate)
            y_pair = (*y_recv, y) if part == 2 else None
            dx, dx_send, dg8, db8, *rest = dx_part(col_arr, grads, (w_own, *wq_oth), x2, x_recv, dy2, dy_recv, stats, g_full, lo, rows, dx, y_pair)
            y = rest[0] if rest else y
            lo += rows
            sums_n.append((dg8, db8))
            dx_recv.append(send(dx_send))
            gate = dx_send
            if part == 0:
                far_a, red_oa, gate = held(far_a, red_oa, gate)
                half_a = (red_oa.astype(F32) + far_a.astype(F32)).astype(BF16)
                rest_a = send(half_a, "depth")
                gate = half_a
            if part == 1:
                far_b, red_ob, gate = held(far_b, red_ob, gate)
                half_b, rest_b = [], []
                for i in range(2):
                    part_rows = slice(0, cut) if i == 0 else slice(cut, None)
                    half_b.append((tie(red_ob, gate)[part_rows].astype(F32) + far_b[part_rows].astype(F32)).astype(BF16))
                    rest_b.append(send(half_b[i], "depth"))
                    gate = half_b[i]

        def natural(pair):
            vals = [jnp.sum(s, axis=0).reshape(3, hw) for s in pair]
            return jnp.concatenate([vals[j][t] for t in range(3) for j in range(2)])

        dg = jnp.sum(sum(pair[0] for pair in sums_n), axis=0)
        dbn = jnp.sum(sum(pair[1] for pair in sums_n), axis=0)
        far = jnp.concatenate([natural(sum_oth), lax.dynamic_slice_in_dim(dg, other * width, width), lax.dynamic_slice_in_dim(dbn, other * width, width)])
        near = jnp.concatenate([natural(sum_own), lax.dynamic_slice_in_dim(dg, col * width, width), lax.dynamic_slice_in_dim(dbn, col * width, width)])
        near = near.reshape(-1, 128)
        far = send(far.reshape(-1, 128))
        far, gate = held(far, gate)
        total = jnp.concatenate([near + far, db_o.reshape(-1, 128)], axis=0)
        row_in = send(total, "row")
        dw_o = (tie(half_o, total).astype(F32) + half_r.astype(F32)).astype(BF16)
        row_in, dw_o = held(row_in, dw_o)
        total = total + row_in
        dep_in = send(total, "depth")
        place, lo = dw_o, 0
        for part, rows in enumerate(parts):
            if part == 3:
                dw_qkv = join(0, piece, dep_arr, half_a, tie(rest_a, dx), half_b[0], rest_b[0], 0, None)
                dw_qkv = join(piece, cut - piece, dep_arr, half_a, rest_a, half_b[0], rest_b[0], 0, dw_qkv)
                place = dw_qkv
            dx = lax.dynamic_update_slice(dx, tie(dx_recv[part], place), (other * half + lo, 0))
            lo += rows
        dw_qkv = join(cut, 2 * piece - cut, dep_arr, half_a, tie(rest_a, dx), half_b[1], rest_b[1], cut, dw_qkv)
        total = total + tie(dep_in, dx)
        db_o = total[-nv:]
        nq = 3 * nv
        return (
            y.reshape(x.shape),
            dx.reshape(x.shape),
            dw_qkv,
            total[:nq],
            dw_o,
            db_o.reshape(-1),
            total[nq:nq + nv].reshape(-1),
            total[nq + nv:nq + 2 * nv].reshape(-1),
        )

    return jax.shard_map(
        block,
        mesh=mesh,
        in_specs=(act_spec, vec_spec, vec_spec, mat_spec, bias_spec, mat_spec, vec_spec, act_spec),
        out_specs=(act_spec, act_spec, mat_spec, bias_spec, mat_spec, vec_spec, vec_spec, vec_spec),
        check_vma=False,
    )
```
